32 devices in a mesh: grp: 4 (over x, core), fsdp: 8 (over z, y).
Axes of the slice: x: 2, y: 2, z: 4, core: 2. Of those that a mesh axis runs over, the one named last changes fastest.
Arguments:
- expert_momentum: float32 [96, 512, 2048], P('grp', 'fsdp'), may hold values from -1500 to 1500
- expert_grad: float32 [96, 512, 2048], P('grp', 'fsdp'), may hold values from -3000 to 3000
- wide_momentum: float32 [4, 2048, 4096], P('grp', None, 'fsdp'), may hold values from -1500 to 1500
- wide_grad: float32 [4, 2048, 4096], P('grp', None, 'fsdp'), may hold values from -3000 to 3000
- assignment: int32 [96], replicated, may hold values from 0 to 7, as said below
- expert_tokens: int32 [96], replicated, may hold values from 16 to 1023
Outputs:
- expert_updates: float32 [96, 512, 2048], P('grp', 'fsdp')
- wide_updates: float32 [4, 2048, 4096], P('grp', None, 'fsdp')
- worker_updates: float32 [32, 6, 512, 2048], P(('grp', 'fsdp'))
The draws below stay inside these ranges and needn't reach their ends.
Inputs may be any that keep to these rules, and one draw needn't show every extreme that they name: `assignment`: within each group of 24 consecutive experts no worker gets more than 6 experts; at least one worker, and possibly several, gets exactly 6.
All inputs are finite; a program needn't handle non-finite values.
Results may differ from the reference program's by a relative error of at most 0.012.
Values may be sent and summed in bfloat16 or wider, within the bound.
No kernel may reach another device: no remote copies, remote signals or barrier semaphores. Data moves between devices by JAX's collectives and lax.ppermute only.
A program may use at most 256 MiB of HBM per device.

```python
import math
import jax
import jax.numpy as jnp
from jax import lax

D = 2048
FE = 512
E = 96
AW = 4096
ITERS = 2
NA = 4
EG = 24
RS = 64
WC = 512
MOST = 6
N_GRP = 4
N_FSDP = 8
DEVICES = 32


def rough(key, lead, rows, cols, base):
    parts = jax.random.split(key, 3)
    core = jnp.clip(jax.random.normal(parts[0], (lead, rows, cols), jnp.float32), -5.0, 5.0)
    stretch = 1.0
    row_scale = jnp.exp(jax.random.uniform(parts[1], (lead, rows, 1), jnp.float32, 0.0, math.log(10.0)))
    col_scale = jnp.exp(jax.random.uniform(parts[2], (lead, 1, cols), jnp.float32, 0.0, math.log(10.0)))
    return base * stretch * core * row_scale * col_scale


def expert_field(key, base):
    field = rough(key, E, FE, D, base)
    flat = (jnp.arange(E) // EG)[:, None, None] * N_FSDP + (jnp.arange(FE) // RS)[None, :, None]
    rising = 3.0 ** (flat.astype(jnp.float32) / (DEVICES - 1))
    return field * rising


def wide_field(key, base):
    field = rough(key, NA, D, AW, base)
    flat = jnp.arange(NA)[:, None, None] * N_FSDP + (jnp.arange(AW) // WC)[None, None, :]
    rising = 3.0 ** (flat.astype(jnp.float32) / (DEVICES - 1))
    return field * rising


def draw_expert_momentum(key, part):
    return expert_field(jax.random.fold_in(key, 11), 0.5)


def draw_expert_grad(key, part):
    return expert_field(jax.random.fold_in(key, 12), 1.0)


def draw_wide_momentum(key, part):
    return wide_field(jax.random.fold_in(key, 13), 0.5)


def draw_wide_grad(key, part):
    return wide_field(jax.random.fold_in(key, 14), 1.0)


def one_group(key):
    parts = jax.random.split(key, 3)
    slot_count = N_FSDP * MOST
    owner = jnp.arange(slot_count, dtype=jnp.int32) // MOST
    chosen = jax.random.randint(parts[0], (), 0, N_FSDP)
    ranking = jax.random.permutation(parts[1], slot_count).astype(jnp.int32)
    score = jnp.where(owner == chosen, jnp.arange(slot_count, dtype=jnp.int32) % MOST - slot_count, ranking)
    picked = jnp.argsort(score, stable=True)
    workers = owner[picked][:EG]
    shuffle = jax.random.permutation(parts[2], EG)
    return workers[shuffle]


def draw_assignment(key, part):
    keys = jax.random.split(jax.random.fold_in(key, 15), E // EG)
    return jax.vmap(one_group)(keys).reshape(E).astype(jnp.int32)


def plant(values, stream_key, smallest, high):
    longest = values.shape.index(max(values.shape))
    spots = []
    for shift in (0, 1):
        where = [jax.random.randint(jax.random.fold_in(stream_key, axis), (), 0, length) for axis, length in enumerate(values.shape)]
        where[longest] = (where[longest] + shift) % values.shape[longest]
        spots.append(tuple(where))
    return values.at[spots[0]].set(smallest).at[spots[1]].set(high)


def setup_inputs(seed: int = 0) -> dict:
    key_of = jax.random.split(jax.random.key(seed), 7)
    return {
        "expert_momentum": draw_expert_momentum(jax.random.fold_in(key_of[6], 71), 0),
        "expert_grad": draw_expert_grad(jax.random.fold_in(key_of[6], 71), 0),
        "wide_momentum": draw_wide_momentum(jax.random.fold_in(key_of[6], 71), 0),
        "wide_grad": draw_wide_grad(jax.random.fold_in(key_of[6], 71), 0),
        "assignment": draw_assignment(jax.random.fold_in(key_of[6], 71), 0),
        "expert_tokens": plant(jax.random.randint(key_of[5], (E,), 16, 1024), jax.random.fold_in(key_of[5], 1), 16, 1023).astype(jnp.int32),
    }


COEF_A = 3.4445
COEF_B = -4.775
COEF_C = 2.0315
BETA = 0.95
EPS = 1e-06

def polish(current, gram):
    gram_low = gram.astype(jnp.bfloat16)
    first = jnp.dot(gram_low, current.astype(jnp.bfloat16), preferred_element_type=jnp.float32)
    second = jnp.dot(gram_low, first.astype(jnp.bfloat16), preferred_element_type=jnp.float32)
    return COEF_A * current + COEF_B * first + COEF_C * second

def whole_gram(matrix):
    low = matrix.astype(jnp.bfloat16)
    return jnp.dot(low, low.T, preferred_element_type=jnp.float32)

def block_gram(matrix):
    low = matrix.astype(jnp.bfloat16)
    width = matrix.shape[1] // N_FSDP
    blocks = low.reshape(matrix.shape[0], N_FSDP, width).transpose(1, 0, 2)

    def add_block(summed, block):
        part = jnp.dot(block, block.T, preferred_element_type=jnp.float32).astype(jnp.bfloat16)
        part = lax.optimization_barrier(part)
        return (summed + part.astype(jnp.float32), None)
    start = jnp.zeros((matrix.shape[0], matrix.shape[0]), jnp.float32)
    summed, unused = lax.scan(add_block, start, blocks)
    return summed

def newton_schulz(merged, gram_fn):
    current = merged
    for step in range(ITERS):
        if step == 0:
            summed = gram_fn(merged)
            norm_sq = jnp.trace(summed) + EPS
            current = merged / jnp.sqrt(norm_sq)
            gram = summed / norm_sq
        else:
            gram = gram_fn(current)
        current = polish(current, gram)
    return current

def reference(expert_momentum, expert_grad, wide_momentum, wide_grad, assignment, expert_tokens):
    expert_merged = BETA * expert_momentum + expert_grad
    wide_merged = BETA * wide_momentum + wide_grad
    tokens = expert_tokens.astype(jnp.float32)
    factor = jnp.sqrt(tokens / jnp.mean(tokens)) * math.sqrt(D)

    def one_expert(pair):
        return newton_schulz(pair[0], whole_gram) * pair[1]

    def one_wide(matrix):
        return newton_schulz(matrix, block_gram) * math.sqrt(AW)
    expert_updates = lax.map(one_expert, (expert_merged, factor))
    wide_updates = lax.map(one_wide, wide_merged)
    order = jnp.arange(E, dtype=jnp.int32)
    group = order // EG
    earlier = (group[:, None] == group[None, :]) & (assignment[:, None] == assignment[None, :]) & (order[None, :] < order[:, None])
    rank = lax.optimization_barrier(jnp.sum(earlier.astype(jnp.int32), axis=1)).astype(jnp.int32)
    target = ((group * N_FSDP + assignment) * MOST + rank).astype(jnp.int32)
    worker_updates = jnp.zeros((N_GRP * N_FSDP * MOST, FE, D), jnp.float32).at[target].set(expert_updates)
    worker_updates = worker_updates.reshape(N_GRP * N_FSDP, MOST, FE, D)
    return (expert_updates, wide_updates, worker_updates)
```

```python
import functools
import math

import jax
import jax.numpy as jnp
from jax import lax
from jax.experimental import pallas as pl
from jax.experimental.pallas import tpu as pltpu
from jax.sharding import PartitionSpec as P

COEF_A = 3.4445
COEF_B = -4.775
COEF_C = 2.0315
BETA = 0.95
EPS = 1e-06

F16_TOP = 32768.0
SMALLEST = 1e-30
BLOCK = 256

F32 = jnp.float32
BF16 = jnp.bfloat16

SMEM_SPEC = pl.BlockSpec(memory_space=pltpu.SMEM)
ANY_SPEC = pl.BlockSpec(memory_space=pl.ANY)


def dot(left, right):
    return jnp.dot(left, right, preferred_element_type=F32)


def dot_nt(left, right):
    return lax.dot_general(left, right, (((1,), (1,)), ((), ())), preferred_element_type=F32)


def cost(flops, bytes_accessed):
    return pl.CostEstimate(flops=int(flops), bytes_accessed=int(bytes_accessed), transcendentals=0)


def route_kernel(members, most, per_group, base_ref, assign_ref, table_ref, count_ref):
    half_members = members // 2
    base = base_ref[0]
    for i in range(members * most):
        table_ref[i] = per_group - 1
    for j in range(members):
        count_ref[j] = 0

    def own(e, carry):
        worker = assign_ref[base + e]
        rank = count_ref[worker]
        table_ref[worker * most + rank] = e
        count_ref[worker] = rank + 1
        return carry

    lax.fori_loop(0, per_group, own, 0)
    for half in range(2):
        first = half * half_members
        last = first + half_members - 1

        def other(e, carry):
            holder, slot = carry
            worker = assign_ref[base + e]
            mine = jnp.logical_and(worker >= first, worker <= last)
            for _ in range(half_members - 1):
                full = slot >= most
                following = jnp.minimum(holder + 1, last)
                slot = jnp.where(full, count_ref[following], slot)
                holder = jnp.where(full, following, holder)

            @pl.when(jnp.logical_not(mine))
            def _():
                table_ref[holder * most + slot] = e

            return holder, jnp.where(mine, slot, slot + 1)

        lax.fori_loop(0, per_group, other, (jnp.int32(first), count_ref[first]))


def route(base, assignment, members, most, per_group):
    return pl.pallas_call(
        functools.partial(route_kernel, members, most, per_group),
        out_shape=(
            jax.ShapeDtypeStruct((members * most,), jnp.int32),
            jax.ShapeDtypeStruct((members,), jnp.int32),
        ),
        in_specs=[SMEM_SPEC, SMEM_SPEC],
        out_specs=(SMEM_SPEC, SMEM_SPEC),
        name="route",
    )(base, assignment)


def merge_kernel(momentum_ref, grad_ref, scaled_ref, top_ref):
    merged = BETA * momentum_ref[...] + grad_ref[...]
    top = jnp.maximum(jnp.max(jnp.abs(merged), axis=(1, 2), keepdims=True), SMALLEST)
    scaled_ref[...] = merged * (F16_TOP / top)
    top_ref[...] = jnp.broadcast_to(top, top_ref.shape)


def merge(momentum, grad):
    per_group, rows, width = momentum.shape
    spec = pl.BlockSpec((1, rows, width), lambda i: (i, 0, 0))
    return pl.pallas_call(
        merge_kernel,
        grid=(per_group,),
        out_shape=(
            jax.ShapeDtypeStruct(momentum.shape, F32),
            jax.ShapeDtypeStruct((per_group, 8, 128), F32),
        ),
        in_specs=[spec, spec],
        out_specs=(spec, pl.BlockSpec((1, 8, 128), lambda i: (i, 0, 0))),
        name="merge",
        cost_estimate=cost(5 * momentum.size, momentum.size * 12),
    )(momentum, grad)


def solve_kernel(
    members, half_members, first_slot,
    row_ref, scale_ref, keep_ref, factor_ref, data_ref, *rest,
):
    work_ref, back_ref, whole, low = rest[-4:]
    rows = data_ref.shape[2]
    size, width = whole.shape
    slot = first_slot + pl.program_id(0)
    tile = min(512, width)

    for member in range(members):
        part = data_ref[member, 0] * scale_ref[slot * members + member]
        whole[pl.ds(member * rows, rows), :] = part
        low[pl.ds(member * rows, rows), :] = part.astype(BF16)

    gram = jnp.zeros((size, size), F32)
    for k in range(width // tile):
        block = low[:, k * tile:(k + 1) * tile]
        gram = gram + dot_nt(block, block)
    row_ids = lax.broadcasted_iota(jnp.int32, (size, size), 0)
    col_ids = lax.broadcasted_iota(jnp.int32, (size, size), 1)
    norm_sq = jnp.sum(jnp.where(row_ids == col_ids, gram, 0.0), keepdims=True) + EPS
    inverse = lax.rsqrt(norm_sq)
    g0 = gram / norm_sq
    g0_low = g0.astype(BF16)
    square = dot(g0_low, g0_low)
    cube = dot(g0_low, square.astype(BF16))
    u = COEF_B * g0 + COEF_C * square
    t = COEF_B * square + COEF_C * cube
    u_low = u.astype(BF16)
    g1 = (COEF_A * COEF_A) * g0 + (2 * COEF_A) * t + dot(u_low, t.astype(BF16))
    g1_low = g1.astype(BF16)
    v = COEF_B * g1 + COEF_C * dot(g1_low, g1_low)
    mix = (COEF_A * (u + v) + dot(v.astype(BF16), u_low)).astype(BF16)
    factor = factor_ref[slot]
    keep = keep_ref[slot]
    for k in range(width // tile):
        cols = slice(k * tile, (k + 1) * tile)
        moved = dot(mix, low[:, cols])
        result = ((COEF_A * COEF_A) * whole[:, cols] + moved) * inverse
        work_ref[0, :, cols] = result * factor
        whole[:, cols] = result * keep
    first_row = pl.multiple_of(row_ref[0], half_members * rows)
    for member in range(half_members):
        back_ref[member, 0] = whole[pl.ds(first_row + member * rows, rows), :]


def solve(first_row, scale, keep, factor, data, work, first_slot, most, half_members):
    members, chunk, rows, width = data.shape
    size = members * rows
    inputs = [first_row, scale, keep, factor, data]
    specs = [SMEM_SPEC] * 4 + [pl.BlockSpec((members, 1, rows, width), lambda i: (0, i, 0, 0))]
    aliases = {}
    if work is not None:
        inputs.append(work)
        specs.append(ANY_SPEC)
        aliases = {5: 0}
    flops = chunk * (4 * size * size * width + 10 * size ** 3)
    return pl.pallas_call(
        functools.partial(solve_kernel, members, half_members, first_slot),
        grid=(chunk,),
        out_shape=(
            jax.ShapeDtypeStruct((most, size, width), F32),
            jax.ShapeDtypeStruct((half_members, chunk, rows, width), F32),
        ),
        in_specs=specs,
        out_specs=(
            pl.BlockSpec((1, size, width), lambda i: (first_slot + i, 0, 0)),
            pl.BlockSpec((half_members, 1, rows, width), lambda i: (0, i, 0, 0)),
        ),
        scratch_shapes=[pltpu.VMEM((size, width), F32), pltpu.VMEM((size, width), BF16)],
        input_output_aliases=aliases,
        name=f"solve{first_slot}",
        cost_estimate=cost(flops, data.size * 12),
    )(*inputs)


def home_kernel(ids_ref, factor_ref, data_ref, *rest):
    rest[-1][...] = data_ref[0] * factor_ref[pl.program_id(0)]


def home(ids, factor, data, out, per_group):
    half_members, chunk, rows, width = data.shape
    inputs = [ids, factor, data]
    specs = [
        SMEM_SPEC,
        pl.BlockSpec((1, 1, rows, width), lambda i, ids: (i // chunk, i % chunk, 0, 0)),
    ]
    aliases = {}
    if out is not None:
        inputs.append(out)
        specs.append(ANY_SPEC)
        aliases = {3: 0}
    return pl.pallas_call(
        home_kernel,
        grid_spec=pltpu.PrefetchScalarGridSpec(
            num_scalar_prefetch=1,
            grid=(half_members * chunk,),
            in_specs=specs,
            out_specs=pl.BlockSpec((1, rows, width), lambda i, ids: (ids[i], 0, 0)),
        ),
        out_shape=jax.ShapeDtypeStruct((per_group, rows, width), F32),
        input_output_aliases=aliases,
        name="home",
        cost_estimate=cost(1e8, data.size * 8),
    )(*inputs)


def wide_gram_kernel(momentum_ref, grad_ref, merged_ref, packed_ref, sum_ref, low):
    i = pl.program_id(0)
    merged = BETA * momentum_ref[...] + grad_ref[...]
    merged_ref[...] = merged
    rounded = merged.astype(BF16)
    low[pl.ds(pl.multiple_of(i * BLOCK, BLOCK), BLOCK), :] = rounded

    @pl.when(i == 0)
    def _():
        sum_ref[...] = jnp.zeros_like(sum_ref)

    squares = jnp.square(rounded.astype(F32))
    sum_ref[...] += jnp.sum(squares, axis=(0, 1), keepdims=True)
    start = i * (i + 1) // 2

    def column(j, carry):
        other = low[pl.ds(pl.multiple_of(j * BLOCK, BLOCK), BLOCK), :]
        place = pl.multiple_of((start + j) * BLOCK, BLOCK)
        packed_ref[pl.ds(place, BLOCK), :] = dot_nt(rounded, other).astype(BF16)
        return carry

    lax.fori_loop(0, i + 1, column, 0)


def wide_gram(momentum, grad):
    height, width = momentum.shape
    number = height // BLOCK
    packed = number * (number + 1) // 2 * BLOCK
    row_spec = pl.BlockSpec((BLOCK, width), lambda i: (i, 0))
    return pl.pallas_call(
        wide_gram_kernel,
        grid=(number,),
        out_shape=(
            jax.ShapeDtypeStruct((height, width), F32),
            jax.ShapeDtypeStruct((packed, BLOCK), BF16),
            jax.ShapeDtypeStruct((8, 128), F32),
        ),
        in_specs=[row_spec, row_spec],
        out_specs=(
            row_spec,
            pl.BlockSpec((packed, BLOCK), lambda i: (0, 0)),
            pl.BlockSpec((8, 128), lambda i: (0, 0)),
        ),
        scratch_shapes=[pltpu.VMEM((height, width), BF16)],
        name="wide_gram",
        cost_estimate=cost(packed * BLOCK * width * 2, height * width * 12 + packed * BLOCK * 2),
    )(momentum, grad)


def wide_solve_kernel(coef_ref, packed_ref, merged_ref, out_ref, gram, first, second, one, two):
    height, width = out_ref.shape
    number = height // BLOCK
    inverse, inverse_sq, outer = coef_ref[0], coef_ref[1], coef_ref[2]

    def assemble(i, carry):
        rows = pl.ds(pl.multiple_of(i * BLOCK, BLOCK), BLOCK)

        def column(j, inner):
            cols = pl.ds(pl.multiple_of(j * BLOCK, BLOCK), BLOCK)
            place = pl.multiple_of((i * (i + 1) // 2 + j) * BLOCK, BLOCK)
            block = packed_ref[pl.ds(place, BLOCK), :]
            gram[cols, rows] = block.T
            gram[rows, cols] = block
            return inner

        return lax.fori_loop(0, i + 1, column, carry)

    lax.fori_loop(0, number, assemble, 0)

    def sweep(source, step):
        def body(i, carry):
            rows = pl.ds(pl.multiple_of(i * BLOCK, BLOCK), BLOCK)
            step(rows, dot(gram[rows, :], source[...]) * inverse_sq)
            return carry

        lax.fori_loop(0, number, body, 0)

    def prepare(i, carry):
        rows = pl.ds(pl.multiple_of(i * BLOCK, BLOCK), BLOCK)
        value = merged_ref[rows, :] * inverse
        first[rows, :] = value
        one[rows, :] = value.astype(BF16)
        return carry

    lax.fori_loop(0, number, prepare, 0)

    def inner_of(base, target):
        def step(rows, product):
            target[rows, :] = (COEF_B * base[rows, :] + COEF_C * product).astype(BF16)
        return step

    def outer_of(base, wide, target):
        def step(rows, product):
            value = COEF_A * base[rows, :] + product
            if wide is not None:
                wide[rows, :] = value
            target[rows, :] = value.astype(BF16)
        return step

    def plain(wide, target):
        def step(rows, product):
            wide[rows, :] = product
            target[rows, :] = product.astype(BF16)
        return step

    sweep(one, inner_of(first, two))
    sweep(two, outer_of(first, first, one))
    sweep(one, inner_of(first, two))
    sweep(two, outer_of(first, None, one))
    sweep(one, plain(second, two))
    sweep(two, inner_of(second, one))

    def turn(rows, product):
        turned = COEF_A * second[rows, :] + product
        value = COEF_B * first[rows, :] + COEF_C * turned
        second[rows, :] = value
        two[rows, :] = value.astype(BF16)

    sweep(one, turn)
    sweep(two, inner_of(second, one))
    sweep(one, outer_of(second, None, two))
    sweep(two, plain(second, one))
    sweep(one, inner_of(second, two))

    def finish(rows, product):
        value = COEF_A * first[rows, :] + COEF_A * second[rows, :] + product
        out_ref[rows, :] = value * outer

    sweep(two, finish)


def wide_solve(coef, packed, merged):
    height, width = merged.shape
    return pl.pallas_call(
        wide_solve_kernel,
        out_shape=jax.ShapeDtypeStruct((height, width), F32),
        in_specs=[SMEM_SPEC] + [pl.BlockSpec(memory_space=pltpu.VMEM)] * 2,
        out_specs=pl.BlockSpec(memory_space=pltpu.VMEM),
        scratch_shapes=[
            pltpu.VMEM((height, height), BF16),
            pltpu.VMEM((height, width), F32),
            pltpu.VMEM((height, width), F32),
            pltpu.VMEM((height, width), BF16),
            pltpu.VMEM((height, width), BF16),
        ],
        name="wide_solve",
        cost_estimate=cost(24 * height * height * width, height * width * 8),
    )(coef, packed, merged)


def on_device(expert_momentum, expert_grad, wide_momentum, wide_grad, assignment, expert_tokens):
    members = lax.axis_size("fsdp")
    half_members = members // 2
    per_group, rows, width = expert_momentum.shape
    wide_height, wide_width = wide_momentum.shape[1:]
    most = 2 * -(-per_group // members)
    chunk = 2
    group_index = lax.axis_index("grp")
    me = lax.axis_index("fsdp")
    half = me // half_members
    halves = [list(range(half_members)), list(range(half_members, members))]
    mirror = [(i, (i + half_members) % members) for i in range(members)]

    def across(value):
        return lax.all_to_all(value, "fsdp", split_axis=0, concat_axis=0, tiled=True)

    def within(value):
        return lax.all_to_all(
            value, "fsdp", split_axis=0, concat_axis=0, tiled=True, axis_index_groups=halves
        )

    base = (group_index * per_group).astype(jnp.int32).reshape(1)
    table, count = route(base, assignment, members, most, per_group)

    wide_merged, packed, squares = wide_gram(wide_momentum[0], wide_grad[0])
    packed_rows = packed.shape[0] // half_members
    parts = within(packed.reshape(half_members, packed_rows, BLOCK))

    scaled, top = merge(expert_momentum, expert_grad)
    slots = table.reshape(members, most)
    outgoing = []
    for start in range(0, most, chunk):
        picked = scaled[slots[:, start:start + chunk].reshape(-1)].astype(jnp.float16)
        outgoing.append(picked.reshape(members, chunk, rows, width))

    notes = jnp.concatenate([top[:, 0, 0], squares[0, :1]])
    notes = jnp.pad(notes, (0, -notes.shape[0] % 128))
    notes = jnp.broadcast_to(notes[None, None, :], (members, 1, notes.shape[0]))
    notes = across(notes)[:, 0]
    arrived = [across(piece) for piece in outgoing]

    part = jnp.sum(parts.astype(F32), axis=0).astype(BF16)
    other = lax.ppermute(part, "fsdp", mirror)
    part = (part.astype(F32) + other.astype(F32)).astype(BF16)
    packed = within(jnp.broadcast_to(part[None], (half_members,) + part.shape))
    packed = packed.reshape(half_members * packed_rows, BLOCK)
    wide_norm = jnp.sum(notes[:, per_group]) + EPS
    coef = jnp.stack(
        [lax.rsqrt(wide_norm), 1.0 / wide_norm, jnp.float32(math.sqrt(wide_width * members))]
    )
    wide_out = wide_solve(coef, packed, wide_merged)

    tops = notes[:, :per_group]
    keep = F16_TOP / jnp.minimum(2.0, jnp.max(tops, axis=0) * 2e7)
    tokens = expert_tokens.astype(F32)
    own_tokens = lax.dynamic_slice_in_dim(tokens, group_index * per_group, per_group)
    factor = jnp.sqrt(own_tokens / jnp.mean(tokens)) * math.sqrt(width)
    own_slots = lax.dynamic_index_in_dim(slots, me, 0, keepdims=False)
    half_slots = lax.dynamic_slice_in_dim(slots, half * half_members, half_members)
    own_count = lax.dynamic_index_in_dim(count, me, 0, keepdims=False)
    own_pick = own_slots[:, None] == jnp.arange(per_group, dtype=jnp.int32)[None, :]
    half_pick = half_slots[:, :, None] == jnp.arange(per_group, dtype=jnp.int32)
    slot_scale = jnp.sum(jnp.where(own_pick[:, None, :], tops[None], 0.0), axis=2) / F16_TOP
    slot_keep = jnp.sum(jnp.where(own_pick, keep[None], 0.0), axis=1)
    slot_factor = jnp.sum(jnp.where(own_pick, factor[None], 0.0), axis=1)
    slot_factor = jnp.where(jnp.arange(most) < own_count, slot_factor, 0.0)
    home_factor = jnp.sum(jnp.where(half_pick, (factor / keep)[None, None], 0.0), axis=2)
    slot_scale = slot_scale.reshape(-1)
    first_row = (half * half_members * rows).astype(jnp.int32).reshape(1)

    work = None
    expert_out = None
    for index, piece in enumerate(arrived):
        start = index * chunk
        work, back = solve(
            first_row, slot_scale, slot_keep, slot_factor, piece.astype(F32), work,
            start, most, half_members,
        )
        back = within(back.astype(jnp.float16)).astype(F32)
        expert_out = home(
            half_slots[:, start:start + chunk].reshape(-1),
            home_factor[:, start:start + chunk].reshape(-1),
            back, expert_out, per_group,
        )
    return (expert_out, wide_out[None], work[None])


def solution(mesh):
    placed = (
        P("grp", "fsdp", None),
        P("grp", "fsdp", None),
        P("grp", None, "fsdp"),
        P("grp", None, "fsdp"),
        P(),
        P(),
    )
    return jax.shard_map(
        on_device,
        mesh=mesh,
        in_specs=placed,
        out_specs=(
            P("grp", "fsdp", None),
            P("grp", None, "fsdp"),
            P(("grp", "fsdp"), None, None, None),
        ),
        check_vma=False,
    )
```

```python
import functools
import math

import jax
import jax.numpy as jnp
from jax import lax
from jax.experimental import pallas as pl
from jax.experimental.pallas import tpu as pltpu
from jax.sharding import PartitionSpec as P


COEF_A = 3.4445
COEF_B = -4.775
COEF_C = 2.0315
BETA = 0.95
EPS = 1e-06

F16_TOP = 32768.0
SMALLEST = 1e-30
BLOCK = 256
PIECE = 128
SWEEP = 512

F32 = jnp.float32
BF16 = jnp.bfloat16

SMEM_SPEC = pl.BlockSpec(memory_space=pltpu.SMEM)
ANY_SPEC = pl.BlockSpec(memory_space=pl.ANY)


def dot(left, right):
    return jnp.dot(left, right, preferred_element_type=F32)


def dot_nt(left, right):
    return lax.dot_general(left, right, (((1,), (1,)), ((), ())), preferred_element_type=F32)


def cost(flops, bytes_accessed):
    return pl.CostEstimate(flops=int(flops), bytes_accessed=int(bytes_accessed), transcendentals=0)


def route_kernel(members, most, per_group, base_ref, assign_ref, table_ref, count_ref):
    half_members = members // 2
    base = base_ref[0]
    for i in range(members * most):
        table_ref[i] = per_group - 1
    for j in range(members):
        count_ref[j] = 0

    def own(e, carry):
        worker = assign_ref[base + e]
        rank = count_ref[worker]
        table_ref[worker * most + rank] = e
        count_ref[worker] = rank + 1
        return carry

    lax.fori_loop(0, per_group, own, 0)
    for half in range(2):
        first = half * half_members
        last = first + half_members - 1

        def other(e, carry):
            holder, slot = carry
            worker = assign_ref[base + e]
            mine = jnp.logical_and(worker >= first, worker <= last)
            for _ in range(half_members - 1):
                full = slot >= most
                following = jnp.minimum(holder + 1, last)
                slot = jnp.where(full, count_ref[following], slot)
                holder = jnp.where(full, following, holder)

            @pl.when(jnp.logical_not(mine))
            def _():
                table_ref[holder * most + slot] = e

            return holder, jnp.where(mine, slot, slot + 1)

        lax.fori_loop(0, per_group, other, (jnp.int32(first), count_ref[first]))


def route(base, assignment, members, most, per_group):
    return pl.pallas_call(
        functools.partial(route_kernel, members, most, per_group),
        out_shape=(
            jax.ShapeDtypeStruct((members * most,), jnp.int32),
            jax.ShapeDtypeStruct((members,), jnp.int32),
        ),
        in_specs=[SMEM_SPEC, SMEM_SPEC],
        out_specs=(SMEM_SPEC, SMEM_SPEC),
        name="route",
    )(base, assignment)


def merge_kernel(momentum_ref, grad_ref, scaled_ref, top_ref):
    for i in range(momentum_ref.shape[0]):
        merged = BETA * momentum_ref[i] + grad_ref[i]
        top = jnp.maximum(jnp.max(jnp.abs(merged), keepdims=True), SMALLEST)
        scaled_ref[i] = merged * (F16_TOP / top)
        top_ref[i] = jnp.broadcast_to(top, top_ref.shape[1:])


def merge(momentum, grad):
    per_group, rows, width = momentum.shape
    step = 4
    spec = pl.BlockSpec((step, rows, width), lambda i: (i, 0, 0))
    return pl.pallas_call(
        merge_kernel,
        grid=(per_group // step,),
        out_shape=(
            jax.ShapeDtypeStruct(momentum.shape, F32),
            jax.ShapeDtypeStruct((per_group, 8, 128), F32),
        ),
        in_specs=[spec, spec],
        out_specs=(spec, pl.BlockSpec((step, 8, 128), lambda i: (i, 0, 0))),
        name="merge",
        cost_estimate=cost(5 * momentum.size, momentum.size * 12),
    )(momentum, grad)


def solve_kernel(
    members, half_members, first_slot,
    row_ref, scale_ref, keep_ref, factor_ref, data_ref, *rest,
):
    work_ref, back_ref, whole, low, held, mixed = rest[-6:]
    rows = data_ref.shape[2]
    size, width = whole.shape
    slot = first_slot + pl.program_id(0)
    tile = min(512, width)

    for member in range(members):
        part = data_ref[member, 0] * scale_ref[slot * members + member]
        whole[pl.ds(member * rows, rows), :] = part
        low[pl.ds(member * rows, rows), :] = part.astype(BF16)

    held[...] = jnp.zeros_like(held)

    def add_gram(k, carry):
        block = low[:, pl.ds(pl.multiple_of(k * tile, tile), tile)]
        held[...] += dot_nt(block, block)
        return carry

    lax.fori_loop(0, width // tile, add_gram, 0)
    gram = held[...]
    row_ids = lax.broadcasted_iota(jnp.int32, (size, size), 0)
    col_ids = lax.broadcasted_iota(jnp.int32, (size, size), 1)
    norm_sq = jnp.sum(jnp.where(row_ids == col_ids, gram, 0.0), keepdims=True) + EPS
    inverse = lax.rsqrt(norm_sq)
    g0 = gram / norm_sq
    g0_low = g0.astype(BF16)
    square = dot(g0_low, g0_low)
    cube = dot(g0_low, square.astype(BF16))
    u = COEF_B * g0 + COEF_C * square
    t = COEF_B * square + COEF_C * cube
    u_low = u.astype(BF16)
    g1 = (COEF_A * COEF_A) * g0 + (2 * COEF_A) * t + dot(u_low, t.astype(BF16))
    g1_low = g1.astype(BF16)
    v = COEF_B * g1 + COEF_C * dot(g1_low, g1_low)
    mix = (COEF_A * (u + v) + dot(v.astype(BF16), u_low)).astype(BF16)
    factor = factor_ref[slot]
    keep = keep_ref[slot]
    mixed[...] = mix

    def apply(k, carry):
        cols = pl.ds(pl.multiple_of(k * tile, tile), tile)
        moved = dot(mixed[...], low[:, cols])
        result = ((COEF_A * COEF_A) * whole[:, cols] + moved) * inverse
        work_ref[0, :, cols] = result * factor
        whole[:, cols] = result * keep
        return carry

    lax.fori_loop(0, width // tile, apply, 0)
    for turn in range(half_members):
        start = pl.multiple_of(row_ref[turn], rows)
        back_ref[turn, 0] = whole[pl.ds(start, rows), :]


def solve(row_starts, scale, keep, factor, data, work, first_slot, most, half_members):
    members, chunk, rows, width = data.shape
    size = members * rows
    inputs = [row_starts, scale, keep, factor, data]
    specs = [SMEM_SPEC] * 4 + [pl.BlockSpec((members, 1, rows, width), lambda i: (0, i, 0, 0))]
    aliases = {}
    if work is not None:
        inputs.append(work)
        specs.append(ANY_SPEC)
        aliases = {5: 0}
    flops = chunk * (4 * size * size * width + 10 * size ** 3)
    return pl.pallas_call(
        functools.partial(solve_kernel, members, half_members, first_slot),
        grid=(chunk,),
        out_shape=(
            jax.ShapeDtypeStruct((most, size, width), F32),
            jax.ShapeDtypeStruct((half_members, chunk, rows, width), F32),
        ),
        in_specs=specs,
        out_specs=(
            pl.BlockSpec((1, size, width), lambda i: (first_slot + i, 0, 0)),
            pl.BlockSpec((half_members, 1, rows, width), lambda i: (0, i, 0, 0)),
        ),
        scratch_shapes=[
            pltpu.VMEM((size, width), F32),
            pltpu.VMEM((size, width), BF16),
            pltpu.VMEM((size, size), F32),
            pltpu.VMEM((size, size), BF16),
        ],
        input_output_aliases=aliases,
        cost_estimate=cost(flops, data.size * 12),
    )(*inputs)


def home_kernel(ids_ref, factor_ref, data_ref, *rest):
    rest[-1][...] = data_ref[0] * factor_ref[pl.program_id(0)]


def home(ids, factor, data, out, per_group):
    half_members, chunk, rows, width = data.shape
    inputs = [ids, factor, data]
    specs = [
        SMEM_SPEC,
        pl.BlockSpec((1, 1, rows, width), lambda i, ids: (i // chunk, i % chunk, 0, 0)),
    ]
    aliases = {}
    if out is not None:
        inputs.append(out)
        specs.append(ANY_SPEC)
        aliases = {3: 0}
    return pl.pallas_call(
        home_kernel,
        grid_spec=pltpu.PrefetchScalarGridSpec(
            num_scalar_prefetch=1,
            grid=(half_members * chunk,),
            in_specs=specs,
            out_specs=pl.BlockSpec((1, rows, width), lambda i, ids: (ids[i], 0, 0)),
        ),
        out_shape=jax.ShapeDtypeStruct((per_group, rows, width), F32),
        input_output_aliases=aliases,
        name="home",
        cost_estimate=cost(1e8, data.size * 8),
    )(*inputs)


def wide_gram_kernel(momentum_ref, grad_ref, merged_ref, packed_ref, sum_ref, low):
    i = pl.program_id(0)
    merged = BETA * momentum_ref[...] + grad_ref[...]
    merged_ref[...] = merged
    rounded = merged.astype(BF16)
    low[pl.ds(pl.multiple_of(i * BLOCK, BLOCK), BLOCK), :] = rounded

    @pl.when(i == 0)
    def _():
        sum_ref[...] = jnp.zeros_like(sum_ref)

    squares = jnp.square(rounded.astype(F32))
    sum_ref[...] += jnp.sum(squares, axis=(0, 1), keepdims=True)
    for k in range(low.shape[0] // BLOCK):

        @pl.when(i == k)
        def _(k=k):
            product = dot_nt(rounded, low[:(k + 1) * BLOCK, :]).astype(BF16)
            start = k * (k + 1) // 2
            for j in range(k + 1):
                rows = slice((start + j) * BLOCK, (start + j + 1) * BLOCK)
                packed_ref[rows, :] = product[:, j * BLOCK:(j + 1) * BLOCK]


def wide_gram(momentum, grad):
    height, width = momentum.shape
    number = height // BLOCK
    packed = number * (number + 1) // 2 * BLOCK
    row_spec = pl.BlockSpec((BLOCK, width), lambda i: (i, 0))
    return pl.pallas_call(
        wide_gram_kernel,
        grid=(number,),
        out_shape=(
            jax.ShapeDtypeStruct((height, width), F32),
            jax.ShapeDtypeStruct((packed, BLOCK), BF16),
            jax.ShapeDtypeStruct((8, 128), F32),
        ),
        in_specs=[row_spec, row_spec],
        out_specs=(
            row_spec,
            pl.BlockSpec((packed, BLOCK), lambda i: (0, 0)),
            pl.BlockSpec((8, 128), lambda i: (0, 0)),
        ),
        scratch_shapes=[pltpu.VMEM((height, width), BF16)],
        name="wide_gram",
        cost_estimate=cost(packed * BLOCK * width * 2, height * width * 12 + packed * BLOCK * 2),
    )(momentum, grad)


def wide_solve_kernel(
    coef_ref, turn_ref, table_ref, packed_ref, merged_ref, out_ref, gram, first, second, low
):
    height, _ = out_ref.shape
    number = height // BLOCK
    pieces = packed_ref.shape[1] // PIECE
    inverse, inverse_sq, outer = coef_ref[0], coef_ref[1], coef_ref[2]

    def assemble(i, carry):
        rows = pl.ds(pl.multiple_of(i * BLOCK, BLOCK), BLOCK)

        def column(j, inner):
            cols = pl.ds(pl.multiple_of(j * BLOCK, BLOCK), BLOCK)
            found = []
            for p in range(BLOCK // PIECE):
                piece = (i * (i + 1) // 2 + j) * (BLOCK // PIECE) + p
                place = pl.multiple_of((piece % pieces) * PIECE, PIECE)
                found.append(packed_ref[turn_ref[piece // pieces], pl.ds(place, PIECE), :])
            block = jnp.concatenate(found, axis=0)
            gram[cols, rows] = block.T
            gram[rows, cols] = block
            return inner

        return lax.fori_loop(0, i + 1, column, carry)

    lax.fori_loop(0, number, assemble, 0)

    def prepare(i, carry):
        rows = pl.ds(pl.multiple_of(i * BLOCK, BLOCK), BLOCK)
        value = merged_ref[rows, :] * inverse
        first[rows, :] = value
        second[rows, :] = jnp.zeros_like(value)
        low[0, rows, :] = value.astype(BF16)
        return carry

    lax.fori_loop(0, number, prepare, 0)

    def sweep(step, carry):
        from_first, from_second, from_product = table_ref[step], table_ref[12 + step], table_ref[24 + step]
        now = step % 2

        def body(i, inner):
            rows = pl.ds(pl.multiple_of(i * SWEEP, SWEEP), SWEEP)
            product = dot(gram[rows, :], low[now]) * (inverse_sq * from_product)
            value = product + from_first * first[rows, :] + from_second * second[rows, :]

            @pl.when(step == 1)
            def _():
                first[rows, :] = value

            @pl.when(jnp.logical_or(step == 4, jnp.logical_or(step == 6, step == 9)))
            def _():
                second[rows, :] = value

            @pl.when(step == 11)
            def _():
                out_ref[rows, :] = value * outer

            low[1 - now, rows, :] = value.astype(BF16)
            return inner

        return lax.fori_loop(0, height // SWEEP, body, carry)

    lax.fori_loop(0, 12, sweep, 0)


A, B, C = COEF_A, COEF_B, COEF_C
SWEEP_FIRST = (B, A, B, A, 0, 0, B, 0, 0, 0, 0, A)
SWEEP_SECOND = (0, 0, 0, 0, 0, B, C * A, B, A, 0, B, A)
SWEEP_PRODUCT = (C, 1, C, 1, 1, C, C, C, 1, 1, C, 1)


def wide_solve(coef, turns, packed, merged):
    height, width = merged.shape
    table = jnp.asarray(SWEEP_FIRST + SWEEP_SECOND + SWEEP_PRODUCT, F32)
    return pl.pallas_call(
        wide_solve_kernel,
        out_shape=jax.ShapeDtypeStruct((height, width), F32),
        in_specs=[SMEM_SPEC] * 3 + [pl.BlockSpec(memory_space=pltpu.VMEM)] * 2,
        out_specs=pl.BlockSpec(memory_space=pltpu.VMEM),
        scratch_shapes=[
            pltpu.VMEM((height, height), BF16),
            pltpu.VMEM((height, width), F32),
            pltpu.VMEM((height, width), F32),
            pltpu.VMEM((2, height, width), BF16),
        ],
        name="wide_solve",
        cost_estimate=cost(24 * height * height * width, height * width * 8),
    )(coef, turns, table, packed, merged)


def on_device(expert_momentum, expert_grad, wide_momentum, wide_grad, assignment, expert_tokens):
    members = lax.axis_size("fsdp")
    half_members = members // 2
    per_group, rows, width = expert_momentum.shape
    _, wide_width = wide_momentum.shape[1:]
    most = 2 * -(-per_group // members)
    sizes = [1] + [2] * ((most - 2) // 2) + [1]
    starts = [sum(sizes[:i]) for i in range(len(sizes))]
    group_index = lax.axis_index("grp")
    me = lax.axis_index("fsdp")
    half = me // half_members
    place = me % half_members
    mirror = [(i, (i + half_members) % members) for i in range(members)]
    steps = jnp.arange(half_members, dtype=jnp.int32)
    onward = (place + steps) % half_members
    origin = (place + half_members - steps) % half_members

    def across(value):
        return lax.all_to_all(value, "fsdp", split_axis=0, concat_axis=0, tiled=True)

    def shifted(value, turn):
        pairs = [
            (i, i // half_members * half_members + (i + turn) % half_members)
            for i in range(members)
        ]
        return lax.ppermute(value, "fsdp", pairs)

    base = (group_index * per_group).astype(jnp.int32).reshape(1)
    table, count = route(base, assignment, members, most, per_group)
    slots = table.reshape(members, most)

    scaled, top = merge(expert_momentum, expert_grad)
    wide_merged, packed, squares = wide_gram(wide_momentum[0], wide_grad[0])
    notes = jnp.concatenate([top[:, 0, 0], squares[0, :1]])
    notes = jnp.pad(notes, (0, -notes.shape[0] % 128))
    notes = jnp.broadcast_to(notes[None, None, :], (members, 1, notes.shape[0]))
    notes = across(notes)[:, 0]
    arrived = []
    for start, chunk in zip(starts, sizes):
        picked = scaled[slots[:, start:start + chunk].reshape(-1)].astype(jnp.float16)
        arrived.append(across(picked.reshape(members, chunk, rows, width)))

    packed_rows = packed.shape[0] // half_members
    packed = packed.reshape(half_members, packed_rows, BLOCK)
    total = lax.dynamic_index_in_dim(packed, place, 0, keepdims=False).astype(F32)
    for turn in range(1, half_members):
        part = lax.dynamic_index_in_dim(packed, onward[turn], 0, keepdims=False)
        total = total + shifted(part, turn).astype(F32)
    part = total.astype(BF16)
    other = lax.ppermute(part, "fsdp", mirror)
    part = (part.astype(F32) + other.astype(F32)).astype(BF16)
    packed = jnp.stack([part] + [shifted(part, turn) for turn in range(1, half_members)])
    wide_norm = jnp.sum(notes[:, per_group]) + EPS
    coef = jnp.stack(
        [lax.rsqrt(wide_norm), 1.0 / wide_norm, jnp.float32(math.sqrt(wide_width * members))]
    )
    wide_out = wide_solve(coef, origin, packed, wide_merged)

    tops = notes[:, :per_group]
    keep = F16_TOP / jnp.minimum(2.0, jnp.max(tops, axis=0) * 2e7)
    tokens = expert_tokens.astype(F32)
    own_tokens = lax.dynamic_slice_in_dim(tokens, group_index * per_group, per_group)
    factor = jnp.sqrt(own_tokens / jnp.mean(tokens)) * math.sqrt(width)
    own_slots = lax.dynamic_index_in_dim(slots, me, 0, keepdims=False)
    half_slots = slots[half * half_members + origin]
    own_count = lax.dynamic_index_in_dim(count, me, 0, keepdims=False)
    own_pick = own_slots[:, None] == jnp.arange(per_group, dtype=jnp.int32)[None, :]
    half_pick = half_slots[:, :, None] == jnp.arange(per_group, dtype=jnp.int32)
    slot_scale = jnp.sum(jnp.where(own_pick[:, None, :], tops[None], 0.0), axis=2) / F16_TOP
    slot_keep = jnp.sum(jnp.where(own_pick, keep[None], 0.0), axis=1)
    slot_factor = jnp.sum(jnp.where(own_pick, factor[None], 0.0), axis=1)
    slot_factor = jnp.where(jnp.arange(most) < own_count, slot_factor, 0.0)
    home_factor = jnp.sum(jnp.where(half_pick, (factor / keep)[None, None], 0.0), axis=2)
    slot_scale = slot_scale.reshape(-1)
    row_starts = ((half * half_members + onward) * rows).astype(jnp.int32)

    work = None
    expert_out = None
    for index, piece in enumerate(arrived):
        start, chunk = starts[index], sizes[index]
        work, back = solve(
            row_starts, slot_scale, slot_keep, slot_factor, piece.astype(F32), work,
            start, most, half_members,
        )
        pieces = [back[0]]
        for turn in range(1, half_members):
            pieces.append(shifted(back[turn].astype(jnp.float16), turn).astype(F32))
        back = jnp.stack(pieces)
        expert_out = home(
            half_slots[:, start:start + chunk].reshape(-1),
            home_factor[:, start:start + chunk].reshape(-1),
            back, expert_out, per_group,
        )
    return (expert_out, wide_out[None], work[None])


def solution(mesh):
    placed = (
        P("grp", "fsdp", None),
        P("grp", "fsdp", None),
        P("grp", None, "fsdp"),
        P("grp", None, "fsdp"),
        P(),
        P(),
    )
    return jax.shard_map(
        on_device,
        mesh=mesh,
        in_specs=placed,
        out_specs=(
            P("grp", "fsdp", None),
            P("grp", None, "fsdp"),
            P(("grp", "fsdp"), None, None, None),
        ),
        check_vma=False,
    )
```

```python
import functools
import math

import jax
import jax.numpy as jnp
from jax import lax
from jax.experimental import pallas as pl
from jax.experimental.pallas import tpu as pltpu
from jax.sharding import PartitionSpec as P


COEF_A = 3.4445
COEF_B = -4.775
COEF_C = 2.0315
BETA = 0.95
EPS = 1e-06

F16_TOP = 32768.0
SMALLEST = 1e-30
BLOCK = 256
PIECE = 128
SWEEP = 512

F32 = jnp.float32
BF16 = jnp.bfloat16

SMEM_SPEC = pl.BlockSpec(memory_space=pltpu.SMEM)
ANY_SPEC = pl.BlockSpec(memory_space=pl.ANY)


def dot(left, right):
    return jnp.dot(left, right, preferred_element_type=F32)


def dot_nt(left, right):
    return lax.dot_general(left, right, (((1,), (1,)), ((), ())), preferred_element_type=F32)


def cost(flops, bytes_accessed):
    return pl.CostEstimate(flops=int(flops), bytes_accessed=int(bytes_accessed), transcendentals=0)


def route_kernel(members, most, per_group, base_ref, assign_ref, table_ref, count_ref):
    half_members = members // 2
    base = base_ref[0]
    for i in range(members * most):
        table_ref[i] = per_group - 1
    for j in range(members):
        count_ref[j] = 0

    def own(e, carry):
        worker = assign_ref[base + e]
        rank = count_ref[worker]
        table_ref[worker * most + rank] = e
        count_ref[worker] = rank + 1
        return carry

    lax.fori_loop(0, per_group, own, 0)
    for half in range(2):
        first = half * half_members
        last = first + half_members - 1

        def other(e, carry):
            holder, slot = carry
            worker = assign_ref[base + e]
            mine = jnp.logical_and(worker >= first, worker <= last)
            for _ in range(half_members - 1):
                full = slot >= most
                following = jnp.minimum(holder + 1, last)
                slot = jnp.where(full, count_ref[following], slot)
                holder = jnp.where(full, following, holder)

            @pl.when(jnp.logical_not(mine))
            def _():
                table_ref[holder * most + slot] = e

            return holder, jnp.where(mine, slot, slot + 1)

        lax.fori_loop(0, per_group, other, (jnp.int32(first), count_ref[first]))


def route(base, assignment, members, most, per_group):
    return pl.pallas_call(
        functools.partial(route_kernel, members, most, per_group),
        out_shape=(
            jax.ShapeDtypeStruct((members * most,), jnp.int32),
            jax.ShapeDtypeStruct((members,), jnp.int32),
        ),
        in_specs=[SMEM_SPEC, SMEM_SPEC],
        out_specs=(SMEM_SPEC, SMEM_SPEC),
        name="route",
    )(base, assignment)


def merge_kernel(momentum_ref, grad_ref, scaled_ref, top_ref):
    for i in range(momentum_ref.shape[0]):
        merged = BETA * momentum_ref[i] + grad_ref[i]
        top = jnp.maximum(jnp.max(jnp.abs(merged), keepdims=True), SMALLEST)
        scaled_ref[i] = merged * (F16_TOP / top)
        top_ref[i] = jnp.broadcast_to(top, top_ref.shape[1:])


def merge(momentum, grad):
    per_group, rows, width = momentum.shape
    step = 4
    spec = pl.BlockSpec((step, rows, width), lambda i: (i, 0, 0))
    return pl.pallas_call(
        merge_kernel,
        grid=(per_group // step,),
        out_shape=(
            jax.ShapeDtypeStruct(momentum.shape, F32),
            jax.ShapeDtypeStruct((per_group, 8, 128), F32),
        ),
        in_specs=[spec, spec],
        out_specs=(spec, pl.BlockSpec((step, 8, 128), lambda i: (i, 0, 0))),
        name="merge",
        cost_estimate=cost(5 * momentum.size, momentum.size * 12),
    )(momentum, grad)


def solve_kernel(
    members, half_members, first_slot,
    row_ref, scale_ref, keep_ref, factor_ref, ratio_ref, data_ref, *rest,
):
    work_ref, back_ref, whole, low = rest[-4:]
    rows = data_ref.shape[2]
    size, width = whole.shape
    slot = first_slot + pl.program_id(0)
    tile = min(512, width)

    for member in range(members):
        part = data_ref[member, 0] * scale_ref[slot * members + member]
        whole[pl.ds(member * rows, rows), :] = part
        low[pl.ds(member * rows, rows), :] = part.astype(BF16)

    gram = jnp.zeros((size, size), F32)
    for k in range(width // tile):
        block = low[:, k * tile:(k + 1) * tile]
        gram = gram + dot_nt(block, block)
    row_ids = lax.broadcasted_iota(jnp.int32, (size, size), 0)
    col_ids = lax.broadcasted_iota(jnp.int32, (size, size), 1)
    norm_sq = jnp.sum(jnp.where(row_ids == col_ids, gram, 0.0), keepdims=True) + EPS
    inverse = lax.rsqrt(norm_sq)
    g0 = gram / norm_sq
    g0_low = g0.astype(BF16)
    square = dot(g0_low, g0_low)
    cube = dot(g0_low, square.astype(BF16))
    u = COEF_B * g0 + COEF_C * square
    t = COEF_B * square + COEF_C * cube
    u_low = u.astype(BF16)
    g1 = (COEF_A * COEF_A) * g0 + (2 * COEF_A) * t + dot(u_low, t.astype(BF16))
    g1_low = g1.astype(BF16)
    v = COEF_B * g1 + COEF_C * dot(g1_low, g1_low)
    mix = (COEF_A * (u + v) + dot(v.astype(BF16), u_low)).astype(BF16)
    factor = factor_ref[slot]
    keep = keep_ref[slot]
    for k in range(width // tile):
        cols = slice(k * tile, (k + 1) * tile)
        moved = dot(mix, low[:, cols])
        result = ((COEF_A * COEF_A) * whole[:, cols] + moved) * inverse
        work_ref[0, :, cols] = result * factor
        whole[:, cols] = result * keep
    for turn in range(half_members):
        start = pl.multiple_of(row_ref[turn], rows)
        block = whole[pl.ds(start, rows), :]
        back_ref[turn, 0] = block * ratio_ref[slot] if turn == 0 else block


def solve(row_starts, scale, keep, factor, ratio, data, work, first_slot, most, half_members):
    members, chunk, rows, width = data.shape
    size = members * rows
    inputs = [row_starts, scale, keep, factor, ratio, data]
    specs = [SMEM_SPEC] * 5 + [pl.BlockSpec((members, 1, rows, width), lambda i: (0, i, 0, 0))]
    aliases = {}
    if work is not None:
        inputs.append(work)
        specs.append(ANY_SPEC)
        aliases = {6: 0}
    flops = chunk * (4 * size * size * width + 10 * size ** 3)
    return pl.pallas_call(
        functools.partial(solve_kernel, members, half_members, first_slot),
        grid=(chunk,),
        out_shape=(
            jax.ShapeDtypeStruct((most, size, width), F32),
            jax.ShapeDtypeStruct((half_members, chunk, rows, width), F32),
        ),
        in_specs=specs,
        out_specs=(
            pl.BlockSpec((1, size, width), lambda i: (first_slot + i, 0, 0)),
            pl.BlockSpec((half_members, 1, rows, width), lambda i: (0, i, 0, 0)),
        ),
        scratch_shapes=[
            pltpu.VMEM((size, width), F32),
            pltpu.VMEM((size, width), BF16),
        ],
        input_output_aliases=aliases,
        cost_estimate=cost(flops, data.size * 12),
    )(*inputs)


def home_kernel(half_members, ids_ref, local_ref, *rest):
    received = rest[:half_members - 1]
    out_ref, held, in_sem, out_sem = rest[-4:]
    chunk = local_ref.shape[1]
    loads, stores = [], []
    for turn in range(half_members):
        for slot in range(chunk):
            i = turn * chunk + slot
            source = received[turn - 1].at[slot] if turn else local_ref.at[0, slot]
            loads.append(pltpu.make_async_copy(source, held.at[i], in_sem.at[i]))
            loads[-1].start()
    for i, load in enumerate(loads):
        load.wait()
        stores.append(pltpu.make_async_copy(held.at[i], out_ref.at[ids_ref[i]], out_sem.at[i]))
        stores[-1].start()
    for store in stores:
        store.wait()


def home(ids, local, received, out, per_group):
    half_members, chunk, rows, width = local.shape
    number = half_members * chunk
    inputs = [ids, local] + received
    aliases = {}
    if out is not None:
        aliases = {len(inputs): 0}
        inputs.append(out)
    return pl.pallas_call(
        functools.partial(home_kernel, half_members),
        in_specs=[SMEM_SPEC] + [ANY_SPEC] * (len(inputs) - 1),
        out_specs=ANY_SPEC,
        out_shape=jax.ShapeDtypeStruct((per_group, rows, width), F32),
        scratch_shapes=[
            pltpu.VMEM((number, rows, width), F32),
            pltpu.SemaphoreType.DMA((number,)),
            pltpu.SemaphoreType.DMA((number,)),
        ],
        input_output_aliases=aliases,
        name="home",
        cost_estimate=cost(2e9, number * rows * width * 8),
    )(*inputs)


def wide_gram_kernel(momentum_ref, grad_ref, merged_ref, packed_ref, sum_ref, low):
    i = pl.program_id(0)
    merged = BETA * momentum_ref[...] + grad_ref[...]
    merged_ref[...] = merged
    rounded = merged.astype(BF16)
    low[pl.ds(pl.multiple_of(i * BLOCK, BLOCK), BLOCK), :] = rounded

    @pl.when(i == 0)
    def _():
        sum_ref[...] = jnp.zeros_like(sum_ref)

    squares = jnp.square(rounded.astype(F32))
    sum_ref[...] += jnp.sum(squares, axis=(0, 1), keepdims=True)
    start = i * (i + 1) // 2

    def columns(j, carry):
        other = low[pl.ds(pl.multiple_of(j * (2 * BLOCK), 2 * BLOCK), 2 * BLOCK), :]
        product = dot_nt(rounded, other).astype(BF16)
        for k in range(2):
            place = pl.multiple_of((start + 2 * j + k) * BLOCK, BLOCK)
            packed_ref[pl.ds(place, BLOCK), :] = product[:, k * BLOCK:(k + 1) * BLOCK]
        return carry

    lax.fori_loop(0, (i + 2) // 2, columns, 0)


def wide_gram(momentum, grad):
    height, width = momentum.shape
    number = height // BLOCK
    packed = number * (number + 1) // 2 * BLOCK
    row_spec = pl.BlockSpec((BLOCK, width), lambda i: (i, 0))
    return pl.pallas_call(
        wide_gram_kernel,
        grid=(number,),
        out_shape=(
            jax.ShapeDtypeStruct((height, width), F32),
            jax.ShapeDtypeStruct((packed, BLOCK), BF16),
            jax.ShapeDtypeStruct((8, 128), F32),
        ),
        in_specs=[row_spec, row_spec],
        out_specs=(
            row_spec,
            pl.BlockSpec((packed, BLOCK), lambda i: (0, 0)),
            pl.BlockSpec((8, 128), lambda i: (0, 0)),
        ),
        scratch_shapes=[pltpu.VMEM((height, width), BF16)],
        name="wide_gram",
        cost_estimate=cost(packed * BLOCK * width * 2, height * width * 12 + packed * BLOCK * 2),
    )(momentum, grad)


def wide_solve_kernel(
    coef_ref, turn_ref, table_ref, merged_ref, *rest
):
    out_ref, packed_ref, gram, first, second, low, sem = rest[-7:]
    height, _ = out_ref.shape
    number = height // BLOCK
    pieces = packed_ref.shape[1] // PIECE
    loads = [
        pltpu.make_async_copy(piece, packed_ref.at[i], sem.at[i]) for i, piece in enumerate(rest[:-7])
    ]
    for load in loads:
        load.start()
    inverse, inverse_sq, outer = coef_ref[0], coef_ref[1], coef_ref[2]

    def prepare(i, carry):
        rows = pl.ds(pl.multiple_of(i * BLOCK, BLOCK), BLOCK)
        value = merged_ref[rows, :] * inverse
        first[rows, :] = value
        second[rows, :] = jnp.zeros_like(value)
        low[0, rows, :] = value.astype(BF16)
        return carry

    lax.fori_loop(0, number, prepare, 0)

    for load in loads:
        load.wait()

    def assemble(i, carry):
        rows = pl.ds(pl.multiple_of(i * BLOCK, BLOCK), BLOCK)

        def column(j, inner):
            cols = pl.ds(pl.multiple_of(j * BLOCK, BLOCK), BLOCK)
            found = []
            for p in range(BLOCK // PIECE):
                piece = (i * (i + 1) // 2 + j) * (BLOCK // PIECE) + p
                place = pl.multiple_of((piece % pieces) * PIECE, PIECE)
                found.append(packed_ref[turn_ref[piece // pieces], pl.ds(place, PIECE), :])
            block = jnp.concatenate(found, axis=0)
            gram[cols, rows] = block.T
            gram[rows, cols] = block
            return inner

        return lax.fori_loop(0, i + 1, column, carry)

    lax.fori_loop(0, number, assemble, 0)

    def sweep(step, carry):
        from_first, from_second, from_product = table_ref[step], table_ref[12 + step], table_ref[24 + step]
        now = step % 2

        def body(i, inner):
            rows = pl.ds(pl.multiple_of(i * SWEEP, SWEEP), SWEEP)
            product = dot(gram[rows, :], low[now]) * (inverse_sq * from_product)
            value = product + from_first * first[rows, :] + from_second * second[rows, :]

            @pl.when(step == 1)
            def _():
                first[rows, :] = value

            @pl.when(jnp.logical_or(step == 4, jnp.logical_or(step == 6, step == 9)))
            def _():
                second[rows, :] = value

            @pl.when(step == 11)
            def _():
                out_ref[rows, :] = value * outer

            low[1 - now, rows, :] = value.astype(BF16)
            return inner

        return lax.fori_loop(0, height // SWEEP, body, carry)

    lax.fori_loop(0, 12, sweep, 0)


A, B, C = COEF_A, COEF_B, COEF_C
SWEEP_FIRST = (B, A, B, A, 0, 0, B, 0, 0, 0, 0, A)
SWEEP_SECOND = (0, 0, 0, 0, 0, B, C * A, B, A, 0, B, A)
SWEEP_PRODUCT = (C, 1, C, 1, 1, C, C, C, 1, 1, C, 1)


def wide_solve(coef, turns, packed, merged):
    height, width = merged.shape
    number = len(packed)
    table = jnp.asarray(SWEEP_FIRST + SWEEP_SECOND + SWEEP_PRODUCT, F32)
    return pl.pallas_call(
        wide_solve_kernel,
        out_shape=jax.ShapeDtypeStruct((height, width), F32),
        in_specs=[SMEM_SPEC] * 3 + [pl.BlockSpec(memory_space=pltpu.VMEM)] + [ANY_SPEC] * number,
        out_specs=pl.BlockSpec(memory_space=pltpu.VMEM),
        scratch_shapes=[
            pltpu.VMEM((number,) + packed[0].shape, BF16),
            pltpu.VMEM((height, height), BF16),
            pltpu.VMEM((height, width), F32),
            pltpu.VMEM((height, width), F32),
            pltpu.VMEM((2, height, width), BF16),
            pltpu.SemaphoreType.DMA((number,)),
        ],
        name="wide_solve",
        cost_estimate=cost(24 * height * height * width, height * width * 8),
    )(coef, turns, table, merged, *packed)


def on_device(expert_momentum, expert_grad, wide_momentum, wide_grad, assignment, expert_tokens):
    members = lax.axis_size("fsdp")
    half_members = members // 2
    per_group, rows, width = expert_momentum.shape
    _, wide_width = wide_momentum.shape[1:]
    most = 2 * -(-per_group // members)
    sizes = [2, 1] * (most // 3) + [1] * (most % 3)
    starts = [sum(sizes[:i]) for i in range(len(sizes))]
    group_index = lax.axis_index("grp")
    me = lax.axis_index("fsdp")
    half = me // half_members
    place = me % half_members
    mirror = [(i, (i + half_members) % members) for i in range(members)]
    steps = jnp.arange(half_members, dtype=jnp.int32)
    onward = (place + steps) % half_members
    origin = (place + half_members - steps) % half_members

    def across(value):
        return lax.all_to_all(value, "fsdp", split_axis=0, concat_axis=0, tiled=True)

    def shifted(value, turn):
        pairs = [
            (i, i // half_members * half_members + (i + turn) % half_members)
            for i in range(members)
        ]
        return lax.ppermute(value, "fsdp", pairs)

    base = (group_index * per_group).astype(jnp.int32).reshape(1)
    table, count = route(base, assignment, members, most, per_group)
    slots = table.reshape(members, most)

    scaled, top = merge(expert_momentum, expert_grad)
    wide_merged, packed, squares = wide_gram(wide_momentum[0], wide_grad[0])
    notes = jnp.concatenate([top[:, 0, 0], squares[0, :1]])
    notes = jnp.pad(notes, (0, -notes.shape[0] % 128))
    notes = jnp.broadcast_to(notes[None, None, :], (members, 1, notes.shape[0]))
    notes = across(notes)[:, 0]
    coded = lax.optimization_barrier(scaled.astype(jnp.float16))
    arrived = []
    for start, chunk in zip(starts, sizes):
        picked = coded[slots[:, start:start + chunk].reshape(-1)]
        arrived.append(across(picked.reshape(members, chunk, rows, width)))

    packed_rows = packed.shape[0] // half_members
    packed = packed.reshape(half_members, packed_rows, BLOCK)
    total = lax.dynamic_index_in_dim(packed, place, 0, keepdims=False).astype(F32)
    for turn in range(1, half_members):
        part = lax.dynamic_index_in_dim(packed, onward[turn], 0, keepdims=False)
        total = total + shifted(part, turn).astype(F32)
    part = total.astype(BF16)
    other = lax.ppermute(part, "fsdp", mirror)
    part = (part.astype(F32) + other.astype(F32)).astype(BF16)
    packed = [part] + [shifted(part, turn) for turn in range(1, half_members)]
    wide_norm = jnp.sum(notes[:, per_group]) + EPS
    coef = jnp.stack(
        [lax.rsqrt(wide_norm), 1.0 / wide_norm, jnp.float32(math.sqrt(wide_width * members))]
    )
    wide_out = wide_solve(coef, origin, packed, wide_merged)

    tops = notes[:, :per_group]
    keep = F16_TOP / jnp.minimum(2.0, jnp.max(tops, axis=0) * 2e7)
    tokens = expert_tokens.astype(F32)
    own_tokens = lax.dynamic_slice_in_dim(tokens, group_index * per_group, per_group)
    factor = jnp.sqrt(own_tokens / jnp.mean(tokens)) * math.sqrt(width)
    own_slots = lax.dynamic_index_in_dim(slots, me, 0, keepdims=False)
    half_slots = slots[half * half_members + origin]
    own_count = lax.dynamic_index_in_dim(count, me, 0, keepdims=False)
    own_pick = own_slots[:, None] == jnp.arange(per_group, dtype=jnp.int32)[None, :]
    half_pick = half_slots[:, :, None] == jnp.arange(per_group, dtype=jnp.int32)
    slot_scale = jnp.sum(jnp.where(own_pick[:, None, :], tops[None], 0.0), axis=2) / F16_TOP
    slot_keep = jnp.sum(jnp.where(own_pick, keep[None], 0.0), axis=1)
    slot_factor = jnp.sum(jnp.where(own_pick, factor[None], 0.0), axis=1)
    slot_ratio = slot_factor / slot_keep
    slot_factor = jnp.where(jnp.arange(most) < own_count, slot_factor, 0.0)
    home_factor = jnp.sum(jnp.where(half_pick, (factor / keep)[None, None], 0.0), axis=2)
    slot_scale = slot_scale.reshape(-1)
    row_starts = ((half * half_members + onward) * rows).astype(jnp.int32)

    work = None
    expert_out = None
    for index, piece in enumerate(arrived):
        start, chunk = starts[index], sizes[index]
        work, back = solve(
            row_starts, slot_scale, slot_keep, slot_factor, slot_ratio, piece.astype(F32), work,
            start, most, half_members,
        )
        received = []
        for turn in range(1, half_members):
            piece = shifted(back[turn].astype(jnp.float16), turn)
            received.append(piece.astype(F32) * home_factor[turn, start:start + chunk, None, None])
        ids = half_slots[:, start:start + chunk].reshape(-1)
        expert_out = home(ids, back, received, expert_out, per_group)
    return (expert_out, wide_out[None], work[None])


def solution(mesh):
    placed = (
        P("grp", "fsdp", None),
        P("grp", "fsdp", None),
        P("grp", None, "fsdp"),
        P("grp", None, "fsdp"),
        P(),
        P(),
    )
    return jax.shard_map(
        on_device,
        mesh=mesh,
        in_specs=placed,
        out_specs=(
            P("grp", "fsdp", None),
            P("grp", None, "fsdp"),
            P(("grp", "fsdp"), None, None, None),
        ),
        check_vma=False,
    )
```

```python
import functools
import math

import jax
import jax.numpy as jnp
from jax import lax
from jax.experimental import pallas as pl
from jax.experimental.pallas import tpu as pltpu
from jax.sharding import PartitionSpec as P


COEF_A = 3.4445
COEF_B = -4.775
COEF_C = 2.0315
BETA = 0.95
EPS = 1e-06

F16_TOP = 32768.0
SMALLEST = 1e-30
BLOCK = 256
PIECE = 128
SWEEP = 512

F32 = jnp.float32
BF16 = jnp.bfloat16

SMEM_SPEC = pl.BlockSpec(memory_space=pltpu.SMEM)
ANY_SPEC = pl.BlockSpec(memory_space=pl.ANY)


def dot(left, right):
    return jnp.dot(left, right, preferred_element_type=F32)


def dot_nt(left, right):
    return lax.dot_general(left, right, (((1,), (1,)), ((), ())), preferred_element_type=F32)


def cost(flops, bytes_accessed):
    return pl.CostEstimate(flops=int(flops), bytes_accessed=int(bytes_accessed), transcendentals=0)


def route_kernel(members, most, per_group, base_ref, assign_ref, table_ref, count_ref):
    half_members = members // 2
    base = base_ref[0]
    for i in range(members * most):
        table_ref[i] = per_group - 1
    for j in range(members):
        count_ref[j] = 0

    def own(e, carry):
        worker = assign_ref[base + e]
        rank = count_ref[worker]
        table_ref[worker * most + rank] = e
        count_ref[worker] = rank + 1
        return carry

    lax.fori_loop(0, per_group, own, 0)
    for half in range(2):
        first = half * half_members
        last = first + half_members - 1

        def other(e, carry):
            holder, slot = carry
            worker = assign_ref[base + e]
            mine = jnp.logical_and(worker >= first, worker <= last)
            for _ in range(half_members - 1):
                full = slot >= most
                following = jnp.minimum(holder + 1, last)
                slot = jnp.where(full, count_ref[following], slot)
                holder = jnp.where(full, following, holder)

            @pl.when(jnp.logical_not(mine))
            def _():
                table_ref[holder * most + slot] = e

            return holder, jnp.where(mine, slot, slot + 1)

        lax.fori_loop(0, per_group, other, (jnp.int32(first), count_ref[first]))


def route(base, assignment, members, most, per_group):
    return pl.pallas_call(
        functools.partial(route_kernel, members, most, per_group),
        out_shape=(
            jax.ShapeDtypeStruct((members * most,), jnp.int32),
            jax.ShapeDtypeStruct((members,), jnp.int32),
        ),
        in_specs=[SMEM_SPEC, SMEM_SPEC],
        out_specs=(SMEM_SPEC, SMEM_SPEC),
        name="route",
    )(base, assignment)


def merge_kernel(momentum_ref, grad_ref, scaled_ref, top_ref):
    for i in range(momentum_ref.shape[0]):
        merged = BETA * momentum_ref[i] + grad_ref[i]
        top = jnp.maximum(jnp.max(jnp.abs(merged), keepdims=True), SMALLEST)
        scaled_ref[i] = merged * (F16_TOP / top)
        top_ref[i] = jnp.broadcast_to(top, top_ref.shape[1:])


def merge(momentum, grad):
    per_group, rows, width = momentum.shape
    step = 4
    spec = pl.BlockSpec((step, rows, width), lambda i: (i, 0, 0))
    return pl.pallas_call(
        merge_kernel,
        grid=(per_group // step,),
        out_shape=(
            jax.ShapeDtypeStruct(momentum.shape, F32),
            jax.ShapeDtypeStruct((per_group, 8, 128), F32),
        ),
        in_specs=[spec, spec],
        out_specs=(spec, pl.BlockSpec((step, 8, 128), lambda i: (i, 0, 0))),
        name="merge",
        cost_estimate=cost(5 * momentum.size, momentum.size * 12),
    )(momentum, grad)


def pick_kernel(table_ref, momentum_ref, grad_ref, scaled_ref):
    merged = BETA * momentum_ref[0] + grad_ref[0]
    top = jnp.maximum(jnp.max(jnp.abs(merged), keepdims=True), SMALLEST)
    scaled_ref[0, 0] = merged * (F16_TOP / top)


def pick_first(table, momentum, grad, members, most, chunk):
    rows, width = momentum.shape[1:]
    source = pl.BlockSpec(
        (1, rows, width), lambda i, table: (table[i // chunk * most + i % chunk], 0, 0)
    )
    return pl.pallas_call(
        pick_kernel,
        grid_spec=pltpu.PrefetchScalarGridSpec(
            num_scalar_prefetch=1,
            grid=(members * chunk,),
            in_specs=[source, source],
            out_specs=pl.BlockSpec(
                (1, 1, rows, width), lambda i, table: (i // chunk, i % chunk, 0, 0)
            ),
        ),
        out_shape=jax.ShapeDtypeStruct((members, chunk, rows, width), F32),
        name="pick_first",
        cost_estimate=cost(2e9, members * chunk * rows * width * 12),
    )(table, momentum, grad)


def solve_kernel(
    members, half_members, first_slot,
    row_ref, scale_ref, keep_ref, factor_ref, ratio_ref, data_ref, *rest,
):
    work_ref, back_ref, whole, low = rest[-4:]
    rows = data_ref.shape[2]
    size, width = whole.shape
    slot = first_slot + pl.program_id(0)
    tile = min(512, width)

    for member in range(members):
        part = data_ref[member, 0] * scale_ref[slot * members + member]
        whole[pl.ds(member * rows, rows), :] = part
        low[pl.ds(member * rows, rows), :] = part.astype(BF16)

    gram = jnp.zeros((size, size), F32)
    for k in range(width // tile):
        block = low[:, k * tile:(k + 1) * tile]
        gram = gram + dot_nt(block, block)
    row_ids = lax.broadcasted_iota(jnp.int32, (size, size), 0)
    col_ids = lax.broadcasted_iota(jnp.int32, (size, size), 1)
    norm_sq = jnp.sum(jnp.where(row_ids == col_ids, gram, 0.0), keepdims=True) + EPS
    inverse = lax.rsqrt(norm_sq)
    g0 = gram / norm_sq
    g0_low = g0.astype(BF16)
    square = dot(g0_low, g0_low)
    cube = dot(g0_low, square.astype(BF16))
    u = COEF_B * g0 + COEF_C * square
    t = COEF_B * square + COEF_C * cube
    u_low = u.astype(BF16)
    g1 = (COEF_A * COEF_A) * g0 + (2 * COEF_A) * t + dot(u_low, t.astype(BF16))
    g1_low = g1.astype(BF16)
    v = COEF_B * g1 + COEF_C * dot(g1_low, g1_low)
    mix = (COEF_A * (u + v) + dot(v.astype(BF16), u_low)).astype(BF16)
    factor = factor_ref[slot]
    keep = keep_ref[slot]
    for k in range(width // tile):
        cols = slice(k * tile, (k + 1) * tile)
        moved = dot(mix, low[:, cols])
        result = ((COEF_A * COEF_A) * whole[:, cols] + moved) * inverse
        work_ref[0, :, cols] = result * factor
        whole[:, cols] = result * keep
    for turn in range(half_members):
        start = pl.multiple_of(row_ref[turn], rows)
        block = whole[pl.ds(start, rows), :]
        back_ref[turn, 0] = block * ratio_ref[slot] if turn == 0 else block


def solve(row_starts, scale, keep, factor, ratio, data, work, first_slot, most, half_members):
    members, chunk, rows, width = data.shape
    size = members * rows
    inputs = [row_starts, scale, keep, factor, ratio, data]
    specs = [SMEM_SPEC] * 5 + [pl.BlockSpec((members, 1, rows, width), lambda i: (0, i, 0, 0))]
    aliases = {}
    if work is not None:
        inputs.append(work)
        specs.append(ANY_SPEC)
        aliases = {6: 0}
    flops = chunk * (4 * size * size * width + 10 * size ** 3)
    return pl.pallas_call(
        functools.partial(solve_kernel, members, half_members, first_slot),
        grid=(chunk,),
        out_shape=(
            jax.ShapeDtypeStruct((most, size, width), F32),
            jax.ShapeDtypeStruct((half_members, chunk, rows, width), F32),
        ),
        in_specs=specs,
        out_specs=(
            pl.BlockSpec((1, size, width), lambda i: (first_slot + i, 0, 0)),
            pl.BlockSpec((half_members, 1, rows, width), lambda i: (0, i, 0, 0)),
        ),
        scratch_shapes=[
            pltpu.VMEM((size, width), F32),
            pltpu.VMEM((size, width), BF16),
        ],
        input_output_aliases=aliases,
        cost_estimate=cost(flops, data.size * 12),
    )(*inputs)


def home_kernel(half_members, ids_ref, local_ref, *rest):
    received = rest[:half_members - 1]
    out_ref, held, in_sem, out_sem = rest[-4:]
    chunk = local_ref.shape[1]
    loads, stores = [], []
    for turn in range(half_members):
        for slot in range(chunk):
            i = turn * chunk + slot
            source = received[turn - 1].at[slot] if turn else local_ref.at[0, slot]
            loads.append(pltpu.make_async_copy(source, held.at[i], in_sem.at[i]))
            loads[-1].start()
    for i, load in enumerate(loads):
        load.wait()
        stores.append(pltpu.make_async_copy(held.at[i], out_ref.at[ids_ref[i]], out_sem.at[i]))
        stores[-1].start()
    for store in stores:
        store.wait()


def home(ids, local, received, out, per_group):
    half_members, chunk, rows, width = local.shape
    number = half_members * chunk
    inputs = [ids, local] + received
    aliases = {}
    if out is not None:
        aliases = {len(inputs): 0}
        inputs.append(out)
    return pl.pallas_call(
        functools.partial(home_kernel, half_members),
        in_specs=[SMEM_SPEC] + [ANY_SPEC] * (len(inputs) - 1),
        out_specs=ANY_SPEC,
        out_shape=jax.ShapeDtypeStruct((per_group, rows, width), F32),
        scratch_shapes=[
            pltpu.VMEM((number, rows, width), F32),
            pltpu.SemaphoreType.DMA((number,)),
            pltpu.SemaphoreType.DMA((number,)),
        ],
        input_output_aliases=aliases,
        name="home",
        cost_estimate=cost(2e9, number * rows * width * 8),
    )(*inputs)


def wide_gram_kernel(momentum_ref, grad_ref, merged_ref, packed_ref, sum_ref, low):
    i = pl.program_id(0)
    step = 2 * BLOCK
    merged = BETA * momentum_ref[...] + grad_ref[...]
    merged_ref[...] = merged
    rounded = merged.astype(BF16)
    low[pl.ds(pl.multiple_of(i * step, step), step), :] = rounded

    @pl.when(i == 0)
    def _():
        sum_ref[...] = jnp.zeros_like(sum_ref)

    squares = jnp.square(rounded.astype(F32))
    sum_ref[...] += jnp.sum(squares, axis=(0, 1), keepdims=True)

    def columns(turn, carry):
        j = i - turn
        other = low[pl.ds(pl.multiple_of(j * step, step), step), :]
        product = dot_nt(rounded, other).astype(BF16)
        for a in range(2):
            row = 2 * i + a
            for b in range(2):
                place = pl.multiple_of((row * (row + 1) // 2 + 2 * j + b) * BLOCK, BLOCK)

                @pl.when(jnp.logical_or(turn > 0, b <= a))
                def _():
                    packed_ref[pl.ds(place, BLOCK), :] = product[
                        a * BLOCK:(a + 1) * BLOCK, b * BLOCK:(b + 1) * BLOCK
                    ]
        return carry

    lax.fori_loop(0, i + 1, columns, 0)


def wide_gram(momentum, grad):
    height, width = momentum.shape
    number = height // BLOCK
    packed = number * (number + 1) // 2 * BLOCK
    row_spec = pl.BlockSpec((2 * BLOCK, width), lambda i: (i, 0))
    return pl.pallas_call(
        wide_gram_kernel,
        grid=(number // 2,),
        out_shape=(
            jax.ShapeDtypeStruct((height, width), F32),
            jax.ShapeDtypeStruct((packed, BLOCK), BF16),
            jax.ShapeDtypeStruct((8, 128), F32),
        ),
        in_specs=[row_spec, row_spec],
        out_specs=(
            row_spec,
            pl.BlockSpec((packed, BLOCK), lambda i: (0, 0)),
            pl.BlockSpec((8, 128), lambda i: (0, 0)),
        ),
        scratch_shapes=[pltpu.VMEM((height, width), BF16)],
        name="wide_gram",
        cost_estimate=cost(packed * BLOCK * width * 2, height * width * 12 + packed * BLOCK * 2),
    )(momentum, grad)


def wide_solve_kernel(
    coef_ref, turn_ref, table_ref, merged_ref, *rest
):
    out_ref, packed_ref, gram, first, second, low, sem = rest[-7:]
    height, _ = out_ref.shape
    number = height // BLOCK
    pieces = packed_ref.shape[1] // PIECE
    loads = [
        pltpu.make_async_copy(piece, packed_ref.at[i], sem.at[i]) for i, piece in enumerate(rest[:-7])
    ]
    for load in loads:
        load.start()
    inverse, inverse_sq, outer = coef_ref[0], coef_ref[1], coef_ref[2]

    def prepare(i, carry):
        rows = pl.ds(pl.multiple_of(i * BLOCK, BLOCK), BLOCK)
        value = merged_ref[rows, :] * inverse
        first[rows, :] = value
        second[rows, :] = jnp.zeros_like(value)
        low[0, rows, :] = value.astype(BF16)
        return carry

    lax.fori_loop(0, number, prepare, 0)

    for load in loads:
        load.wait()

    def assemble(i, carry):
        rows = pl.ds(pl.multiple_of(i * BLOCK, BLOCK), BLOCK)

        def column(j, inner):
            cols = pl.ds(pl.multiple_of(j * BLOCK, BLOCK), BLOCK)
            found = []
            for p in range(BLOCK // PIECE):
                piece = (i * (i + 1) // 2 + j) * (BLOCK // PIECE) + p
                place = pl.multiple_of((piece % pieces) * PIECE, PIECE)
                found.append(packed_ref[turn_ref[piece // pieces], pl.ds(place, PIECE), :])
            block = jnp.concatenate(found, axis=0)
            gram[cols, rows] = block.T
            gram[rows, cols] = block
            return inner

        return lax.fori_loop(0, i + 1, column, carry)

    lax.fori_loop(0, number, assemble, 0)

    def sweep(step, carry):
        from_first, from_second, from_product = table_ref[step], table_ref[12 + step], table_ref[24 + step]
        now = step % 2

        def body(i, inner):
            rows = pl.ds(pl.multiple_of(i * SWEEP, SWEEP), SWEEP)
            product = dot(gram[rows, :], low[now]) * (inverse_sq * from_product)
            value = product + from_first * first[rows, :] + from_second * second[rows, :]

            @pl.when(step == 1)
            def _():
                first[rows, :] = value

            @pl.when(jnp.logical_or(step == 4, jnp.logical_or(step == 6, step == 9)))
            def _():
                second[rows, :] = value

            @pl.when(step == 11)
            def _():
                out_ref[rows, :] = value * outer

            low[1 - now, rows, :] = value.astype(BF16)
            return inner

        return lax.fori_loop(0, height // SWEEP, body, carry)

    lax.fori_loop(0, 12, sweep, 0)


A, B, C = COEF_A, COEF_B, COEF_C
SWEEP_FIRST = (B, A, B, A, 0, 0, B, 0, 0, 0, 0, A)
SWEEP_SECOND = (0, 0, 0, 0, 0, B, C * A, B, A, 0, B, A)
SWEEP_PRODUCT = (C, 1, C, 1, 1, C, C, C, 1, 1, C, 1)


def wide_solve(coef, turns, packed, merged):
    height, width = merged.shape
    number = len(packed)
    table = jnp.asarray(SWEEP_FIRST + SWEEP_SECOND + SWEEP_PRODUCT, F32)
    return pl.pallas_call(
        wide_solve_kernel,
        out_shape=jax.ShapeDtypeStruct((height, width), F32),
        in_specs=[SMEM_SPEC] * 3 + [pl.BlockSpec(memory_space=pltpu.VMEM)] + [ANY_SPEC] * number,
        out_specs=pl.BlockSpec(memory_space=pltpu.VMEM),
        scratch_shapes=[
            pltpu.VMEM((number,) + packed[0].shape, BF16),
            pltpu.VMEM((height, height), BF16),
            pltpu.VMEM((height, width), F32),
            pltpu.VMEM((height, width), F32),
            pltpu.VMEM((2, height, width), BF16),
            pltpu.SemaphoreType.DMA((number,)),
        ],
        name="wide_solve",
        cost_estimate=cost(24 * height * height * width, height * width * 8),
    )(coef, turns, table, merged, *packed)


def on_device(expert_momentum, expert_grad, wide_momentum, wide_grad, assignment, expert_tokens):
    members = lax.axis_size("fsdp")
    half_members = members // 2
    per_group, rows, width = expert_momentum.shape
    _, wide_width = wide_momentum.shape[1:]
    most = 2 * -(-per_group // members)
    sizes = [2, 1] * (most // 3) + [1] * (most % 3)
    starts = [sum(sizes[:i]) for i in range(len(sizes))]
    group_index = lax.axis_index("grp")
    me = lax.axis_index("fsdp")
    half = me // half_members
    place = me % half_members
    mirror = [(i, (i + half_members) % members) for i in range(members)]
    steps = jnp.arange(half_members, dtype=jnp.int32)
    onward = (place + steps) % half_members
    origin = (place + half_members - steps) % half_members

    def across(value):
        return lax.all_to_all(value, "fsdp", split_axis=0, concat_axis=0, tiled=True)

    def shifted(value, turn):
        pairs = [
            (i, i // half_members * half_members + (i + turn) % half_members)
            for i in range(members)
        ]
        return lax.ppermute(value, "fsdp", pairs)

    base = (group_index * per_group).astype(jnp.int32).reshape(1)
    table, count = route(base, assignment, members, most, per_group)
    slots = table.reshape(members, most)

    scaled, top = merge(expert_momentum, expert_grad)
    wide_merged, packed, squares = wide_gram(wide_momentum[0], wide_grad[0])
    notes = jnp.concatenate([top[:, 0, 0], squares[0, :1]])
    notes = jnp.pad(notes, (0, -notes.shape[0] % 128))
    notes = jnp.broadcast_to(notes[None, None, :], (members, 1, notes.shape[0]))
    notes = across(notes)[:, 0]
    coded = lax.optimization_barrier(scaled.astype(jnp.float16))
    arrived = []
    for index, (start, chunk) in enumerate(zip(starts, sizes)):
        if index == 0:
            picked = pick_first(table, expert_momentum, expert_grad, members, most, chunk)
            picked = picked.astype(jnp.float16)
        else:
            picked = coded[slots[:, start:start + chunk].reshape(-1)]
        arrived.append(across(picked.reshape(members, chunk, rows, width)))

    packed_rows = packed.shape[0] // half_members
    packed = packed.reshape(half_members, packed_rows, BLOCK)
    total = lax.dynamic_index_in_dim(packed, place, 0, keepdims=False).astype(F32)
    for turn in range(1, half_members):
        part = lax.dynamic_index_in_dim(packed, onward[turn], 0, keepdims=False)
        total = total + shifted(part, turn).astype(F32)
    part = total.astype(BF16)
    other = lax.ppermute(part, "fsdp", mirror)
    part = (part.astype(F32) + other.astype(F32)).astype(BF16)
    packed = [part] + [shifted(part, turn) for turn in range(1, half_members)]
    wide_norm = jnp.sum(notes[:, per_group]) + EPS
    coef = jnp.stack(
        [lax.rsqrt(wide_norm), 1.0 / wide_norm, jnp.float32(math.sqrt(wide_width * members))]
    )
    wide_out = wide_solve(coef, origin, packed, wide_merged)

    tops = notes[:, :per_group]
    keep = F16_TOP / jnp.minimum(2.0, jnp.max(tops, axis=0) * 2e7)
    tokens = expert_tokens.astype(F32)
    own_tokens = lax.dynamic_slice_in_dim(tokens, group_index * per_group, per_group)
    factor = jnp.sqrt(own_tokens / jnp.mean(tokens)) * math.sqrt(width)
    own_slots = lax.dynamic_index_in_dim(slots, me, 0, keepdims=False)
    half_slots = slots[half * half_members + origin]
    own_count = lax.dynamic_index_in_dim(count, me, 0, keepdims=False)
    own_pick = own_slots[:, None] == jnp.arange(per_group, dtype=jnp.int32)[None, :]
    half_pick = half_slots[:, :, None] == jnp.arange(per_group, dtype=jnp.int32)
    slot_scale = jnp.sum(jnp.where(own_pick[:, None, :], tops[None], 0.0), axis=2) / F16_TOP
    slot_keep = jnp.sum(jnp.where(own_pick, keep[None], 0.0), axis=1)
    slot_factor = jnp.sum(jnp.where(own_pick, factor[None], 0.0), axis=1)
    slot_ratio = slot_factor / slot_keep
    slot_factor = jnp.where(jnp.arange(most) < own_count, slot_factor, 0.0)
    home_factor = jnp.sum(jnp.where(half_pick, (factor / keep)[None, None], 0.0), axis=2)
    slot_scale = slot_scale.reshape(-1)
    row_starts = ((half * half_members + onward) * rows).astype(jnp.int32)

    work = None
    expert_out = None
    for index, piece in enumerate(arrived):
        start, chunk = starts[index], sizes[index]
        work, back = solve(
            row_starts, slot_scale, slot_keep, slot_factor, slot_ratio, piece.astype(F32), work,
            start, most, half_members,
        )
        received = []
        for turn in range(1, half_members):
            piece = shifted(back[turn].astype(jnp.float16), turn)
            received.append(piece.astype(F32) * home_factor[turn, start:start + chunk, None, None])
        ids = half_slots[:, start:start + chunk].reshape(-1)
        expert_out = home(ids, back, received, expert_out, per_group)
    return (expert_out, wide_out[None], work[None])


def solution(mesh):
    placed = (
        P("grp", "fsdp", None),
        P("grp", "fsdp", None),
        P("grp", None, "fsdp"),
        P("grp", None, "fsdp"),
        P(),
        P(),
    )
    return jax.shard_map(
        on_device,
        mesh=mesh,
        in_specs=placed,
        out_specs=(
            P("grp", "fsdp", None),
            P("grp", None, "fsdp"),
            P(("grp", "fsdp"), None, None, None),
        ),
        check_vma=False,
    )
```

```python
import functools
import math

import jax
import jax.numpy as jnp
from jax import lax
from jax.experimental import pallas as pl
from jax.experimental.pallas import tpu as pltpu
from jax.sharding import PartitionSpec as P


COEF_A = 3.4445
COEF_B = -4.775
COEF_C = 2.0315
BETA = 0.95
EPS = 1e-06

F16_TOP = 32768.0
SMALLEST = 1e-30
BLOCK = 256
PIECE = 128
SWEEP = 512

F32 = jnp.float32
BF16 = jnp.bfloat16

SMEM_SPEC = pl.BlockSpec(memory_space=pltpu.SMEM)
ANY_SPEC = pl.BlockSpec(memory_space=pl.ANY)


def dot(left, right):
    return jnp.dot(left, right, preferred_element_type=F32)


def dot_nt(left, right):
    return lax.dot_general(left, right, (((1,), (1,)), ((), ())), preferred_element_type=F32)


def cost(flops, bytes_accessed):
    return pl.CostEstimate(flops=int(flops), bytes_accessed=int(bytes_accessed), transcendentals=0)


def route_kernel(members, most, per_group, base_ref, assign_ref, table_ref, count_ref):
    half_members = members // 2
    base = base_ref[0]
    for i in range(members * most):
        table_ref[i] = per_group - 1
    for j in range(members):
        count_ref[j] = 0

    def own(e, carry):
        worker = assign_ref[base + e]
        rank = count_ref[worker]
        table_ref[worker * most + rank] = e
        count_ref[worker] = rank + 1
        return carry

    lax.fori_loop(0, per_group, own, 0)
    for half in range(2):
        first = half * half_members
        last = first + half_members - 1

        def other(e, carry):
            holder, slot = carry
            worker = assign_ref[base + e]
            mine = jnp.logical_and(worker >= first, worker <= last)
            for _ in range(half_members - 1):
                full = slot >= most
                following = jnp.minimum(holder + 1, last)
                slot = jnp.where(full, count_ref[following], slot)
                holder = jnp.where(full, following, holder)

            @pl.when(jnp.logical_not(mine))
            def _():
                table_ref[holder * most + slot] = e

            return holder, jnp.where(mine, slot, slot + 1)

        lax.fori_loop(0, per_group, other, (jnp.int32(first), count_ref[first]))


def route(base, assignment, members, most, per_group):
    return pl.pallas_call(
        functools.partial(route_kernel, members, most, per_group),
        out_shape=(
            jax.ShapeDtypeStruct((members * most,), jnp.int32),
            jax.ShapeDtypeStruct((members,), jnp.int32),
        ),
        in_specs=[SMEM_SPEC, SMEM_SPEC],
        out_specs=(SMEM_SPEC, SMEM_SPEC),
        name="route",
    )(base, assignment)


def merge_kernel(momentum_ref, grad_ref, scaled_ref, top_ref):
    for i in range(momentum_ref.shape[0]):
        merged = BETA * momentum_ref[i] + grad_ref[i]
        top = jnp.maximum(jnp.max(jnp.abs(merged), keepdims=True), SMALLEST)
        scaled_ref[i] = merged * (F16_TOP / top)
        top_ref[i] = jnp.broadcast_to(top, top_ref.shape[1:])


def merge(momentum, grad):
    per_group, rows, width = momentum.shape
    step = 4
    spec = pl.BlockSpec((step, rows, width), lambda i: (i, 0, 0))
    return pl.pallas_call(
        merge_kernel,
        grid=(per_group // step,),
        out_shape=(
            jax.ShapeDtypeStruct(momentum.shape, F32),
            jax.ShapeDtypeStruct((per_group, 8, 128), F32),
        ),
        in_specs=[spec, spec],
        out_specs=(spec, pl.BlockSpec((step, 8, 128), lambda i: (i, 0, 0))),
        name="merge",
        cost_estimate=cost(5 * momentum.size, momentum.size * 12),
    )(momentum, grad)


def solve_kernel(
    members, half_members, first_slot,
    row_ref, scale_ref, keep_ref, factor_ref, ratio_ref, data_ref, *rest,
):
    work_ref, back_ref, whole, low = rest[-4:]
    rows = data_ref.shape[2]
    size, width = whole.shape
    slot = first_slot + pl.program_id(0)
    tile = min(512, width)

    for member in range(members):
        part = data_ref[member, 0] * scale_ref[slot * members + member]
        whole[pl.ds(member * rows, rows), :] = part
        low[pl.ds(member * rows, rows), :] = part.astype(BF16)

    gram = jnp.zeros((size, size), F32)
    for k in range(width // tile):
        block = low[:, k * tile:(k + 1) * tile]
        gram = gram + dot_nt(block, block)
    row_ids = lax.broadcasted_iota(jnp.int32, (size, size), 0)
    col_ids = lax.broadcasted_iota(jnp.int32, (size, size), 1)
    norm_sq = jnp.sum(jnp.where(row_ids == col_ids, gram, 0.0), keepdims=True) + EPS
    inverse = lax.rsqrt(norm_sq)
    g0 = gram / norm_sq
    g0_low = g0.astype(BF16)
    square = dot(g0_low, g0_low)
    cube = dot(g0_low, square.astype(BF16))
    u = COEF_B * g0 + COEF_C * square
    t = COEF_B * square + COEF_C * cube
    u_low = u.astype(BF16)
    g1 = (COEF_A * COEF_A) * g0 + (2 * COEF_A) * t + dot(u_low, t.astype(BF16))
    g1_low = g1.astype(BF16)
    v = COEF_B * g1 + COEF_C * dot(g1_low, g1_low)
    mix = (COEF_A * (u + v) + dot(v.astype(BF16), u_low)).astype(BF16)
    factor = factor_ref[slot]
    keep = keep_ref[slot]
    for k in range(width // tile):
        cols = slice(k * tile, (k + 1) * tile)
        moved = dot(mix, low[:, cols])
        result = ((COEF_A * COEF_A) * whole[:, cols] + moved) * inverse
        work_ref[0, :, cols] = result * factor
        whole[:, cols] = result * keep
    for turn in range(half_members):
        start = pl.multiple_of(row_ref[turn], rows)
        block = whole[pl.ds(start, rows), :]
        back_ref[turn, 0] = block * ratio_ref[slot] if turn == 0 else block


def solve(row_starts, scale, keep, factor, ratio, data, work, first_slot, most, half_members):
    members, chunk, rows, width = data.shape
    size = members * rows
    inputs = [row_starts, scale, keep, factor, ratio, data]
    specs = [SMEM_SPEC] * 5 + [pl.BlockSpec((members, 1, rows, width), lambda i: (0, i, 0, 0))]
    aliases = {}
    if work is not None:
        inputs.append(work)
        specs.append(ANY_SPEC)
        aliases = {6: 0}
    flops = chunk * (4 * size * size * width + 10 * size ** 3)
    return pl.pallas_call(
        functools.partial(solve_kernel, members, half_members, first_slot),
        grid=(chunk,),
        out_shape=(
            jax.ShapeDtypeStruct((most, size, width), F32),
            jax.ShapeDtypeStruct((half_members, chunk, rows, width), F32),
        ),
        in_specs=specs,
        out_specs=(
            pl.BlockSpec((1, size, width), lambda i: (first_slot + i, 0, 0)),
            pl.BlockSpec((half_members, 1, rows, width), lambda i: (0, i, 0, 0)),
        ),
        scratch_shapes=[
            pltpu.VMEM((size, width), F32),
            pltpu.VMEM((size, width), BF16),
        ],
        input_output_aliases=aliases,
        cost_estimate=cost(flops, data.size * 12),
    )(*inputs)


def home_kernel(half_members, ids_ref, local_ref, *rest):
    received = rest[:half_members - 1]
    out_ref, held, in_sem, out_sem = rest[-4:]
    chunk = local_ref.shape[1]
    loads, stores = [], []
    for turn in range(half_members):
        for slot in range(chunk):
            i = turn * chunk + slot
            source = received[turn - 1].at[slot] if turn else local_ref.at[0, slot]
            loads.append(pltpu.make_async_copy(source, held.at[i], in_sem.at[i]))
            loads[-1].start()
    for i, load in enumerate(loads):
        load.wait()
        stores.append(pltpu.make_async_copy(held.at[i], out_ref.at[ids_ref[i]], out_sem.at[i]))
        stores[-1].start()
    for store in stores:
        store.wait()


def home(ids, local, received, out, per_group):
    half_members, chunk, rows, width = local.shape
    number = half_members * chunk
    inputs = [ids, local] + received
    aliases = {}
    if out is not None:
        aliases = {len(inputs): 0}
        inputs.append(out)
    return pl.pallas_call(
        functools.partial(home_kernel, half_members),
        in_specs=[SMEM_SPEC] + [ANY_SPEC] * (len(inputs) - 1),
        out_specs=ANY_SPEC,
        out_shape=jax.ShapeDtypeStruct((per_group, rows, width), F32),
        scratch_shapes=[
            pltpu.VMEM((number, rows, width), F32),
            pltpu.SemaphoreType.DMA((number,)),
            pltpu.SemaphoreType.DMA((number,)),
        ],
        input_output_aliases=aliases,
        name="home",
        cost_estimate=cost(2e9, number * rows * width * 8),
    )(*inputs)


def wide_gram_kernel(momentum_ref, grad_ref, merged_ref, packed_ref, sum_ref, low):
    i = pl.program_id(0)
    step = 2 * BLOCK
    merged = BETA * momentum_ref[...] + grad_ref[...]
    merged_ref[...] = merged
    rounded = merged.astype(BF16)
    low[pl.ds(pl.multiple_of(i * step, step), step), :] = rounded

    @pl.when(i == 0)
    def _():
        sum_ref[...] = jnp.zeros_like(sum_ref)

    squares = jnp.square(rounded.astype(F32))
    sum_ref[...] += jnp.sum(squares, axis=(0, 1), keepdims=True)

    def columns(turn, carry):
        j = i - turn
        other = low[pl.ds(pl.multiple_of(j * step, step), step), :]
        product = dot_nt(rounded, other).astype(BF16)
        for a in range(2):
            row = 2 * i + a
            for b in range(2):
                place = pl.multiple_of((row * (row + 1) // 2 + 2 * j + b) * BLOCK, BLOCK)

                @pl.when(jnp.logical_or(turn > 0, b <= a))
                def _():
                    packed_ref[pl.ds(place, BLOCK), :] = product[
                        a * BLOCK:(a + 1) * BLOCK, b * BLOCK:(b + 1) * BLOCK
                    ]
        return carry

    lax.fori_loop(0, i + 1, columns, 0)


def wide_gram(momentum, grad):
    height, width = momentum.shape
    number = height // BLOCK
    packed = number * (number + 1) // 2 * BLOCK
    row_spec = pl.BlockSpec((2 * BLOCK, width), lambda i: (i, 0))
    return pl.pallas_call(
        wide_gram_kernel,
        grid=(number // 2,),
        out_shape=(
            jax.ShapeDtypeStruct((height, width), F32),
            jax.ShapeDtypeStruct((packed, BLOCK), BF16),
            jax.ShapeDtypeStruct((8, 128), F32),
        ),
        in_specs=[row_spec, row_spec],
        out_specs=(
            row_spec,
            pl.BlockSpec((packed, BLOCK), lambda i: (0, 0)),
            pl.BlockSpec((8, 128), lambda i: (0, 0)),
        ),
        scratch_shapes=[pltpu.VMEM((height, width), BF16)],
        name="wide_gram",
        cost_estimate=cost(packed * BLOCK * width * 2, height * width * 12 + packed * BLOCK * 2),
    )(momentum, grad)


def wide_solve_kernel(
    coef_ref, turn_ref, table_ref, merged_ref, *rest
):
    out_ref, packed_ref, gram, first, second, low, sem = rest[-7:]
    height, _ = out_ref.shape
    number = height // BLOCK
    pieces = packed_ref.shape[1] // PIECE
    loads = [
        pltpu.make_async_copy(piece, packed_ref.at[i], sem.at[i]) for i, piece in enumerate(rest[:-7])
    ]
    for load in loads:
        load.start()
    inverse, inverse_sq, outer = coef_ref[0], coef_ref[1], coef_ref[2]

    def prepare(i, carry):
        rows = pl.ds(pl.multiple_of(i * BLOCK, BLOCK), BLOCK)
        value = merged_ref[rows, :] * inverse
        first[rows, :] = value
        second[rows, :] = jnp.zeros_like(value)
        low[0, rows, :] = value.astype(BF16)
        return carry

    lax.fori_loop(0, number, prepare, 0)

    for load in loads:
        load.wait()

    def assemble(i, carry):
        rows = pl.ds(pl.multiple_of(i * BLOCK, BLOCK), BLOCK)

        def column(j, inner):
            cols = pl.ds(pl.multiple_of(j * BLOCK, BLOCK), BLOCK)
            found = []
            for p in range(BLOCK // PIECE):
                piece = (i * (i + 1) // 2 + j) * (BLOCK // PIECE) + p
                place = pl.multiple_of((piece % pieces) * PIECE, PIECE)
                found.append(packed_ref[turn_ref[piece // pieces], pl.ds(place, PIECE), :])
            block = jnp.concatenate(found, axis=0)
            gram[cols, rows] = block.T
            gram[rows, cols] = block
            return inner

        return lax.fori_loop(0, i + 1, column, carry)

    lax.fori_loop(0, number, assemble, 0)

    def sweep(step, carry):
        from_first, from_second, from_product = table_ref[step], table_ref[12 + step], table_ref[24 + step]
        now = step % 2

        def body(i, inner):
            rows = pl.ds(pl.multiple_of(i * SWEEP, SWEEP), SWEEP)
            product = dot(gram[rows, :], low[now]) * (inverse_sq * from_product)
            value = product + from_first * first[rows, :] + from_second * second[rows, :]

            @pl.when(step == 1)
            def _():
                first[rows, :] = value

            @pl.when(jnp.logical_or(step == 4, jnp.logical_or(step == 6, step == 9)))
            def _():
                second[rows, :] = value

            @pl.when(step == 11)
            def _():
                out_ref[rows, :] = value * outer

            low[1 - now, rows, :] = value.astype(BF16)
            return inner

        return lax.fori_loop(0, height // SWEEP, body, carry)

    lax.fori_loop(0, 12, sweep, 0)


A, B, C = COEF_A, COEF_B, COEF_C
SWEEP_FIRST = (B, A, B, A, 0, 0, B, 0, 0, 0, 0, A)
SWEEP_SECOND = (0, 0, 0, 0, 0, B, C * A, B, A, 0, B, A)
SWEEP_PRODUCT = (C, 1, C, 1, 1, C, C, C, 1, 1, C, 1)


def wide_solve(coef, turns, packed, merged):
    height, width = merged.shape
    number = len(packed)
    table = jnp.asarray(SWEEP_FIRST + SWEEP_SECOND + SWEEP_PRODUCT, F32)
    return pl.pallas_call(
        wide_solve_kernel,
        out_shape=jax.ShapeDtypeStruct((height, width), F32),
        in_specs=[SMEM_SPEC] * 3 + [pl.BlockSpec(memory_space=pltpu.VMEM)] + [ANY_SPEC] * number,
        out_specs=pl.BlockSpec(memory_space=pltpu.VMEM),
        scratch_shapes=[
            pltpu.VMEM((number,) + packed[0].shape, BF16),
            pltpu.VMEM((height, height), BF16),
            pltpu.VMEM((height, width), F32),
            pltpu.VMEM((height, width), F32),
            pltpu.VMEM((2, height, width), BF16),
            pltpu.SemaphoreType.DMA((number,)),
        ],
        name="wide_solve",
        cost_estimate=cost(24 * height * height * width, height * width * 8),
    )(coef, turns, table, merged, *packed)


def on_device(expert_momentum, expert_grad, wide_momentum, wide_grad, assignment, expert_tokens):
    members = lax.axis_size("fsdp")
    half_members = members // 2
    per_group, rows, width = expert_momentum.shape
    _, wide_width = wide_momentum.shape[1:]
    most = 2 * -(-per_group // members)
    sizes = [1] + [2] * ((most - 2) // 2) + [1]
    starts = [sum(sizes[:i]) for i in range(len(sizes))]
    group_index = lax.axis_index("grp")
    me = lax.axis_index("fsdp")
    half = me // half_members
    place = me % half_members
    mirror = [(i, (i + half_members) % members) for i in range(members)]
    steps = jnp.arange(half_members, dtype=jnp.int32)
    onward = (place + steps) % half_members
    origin = (place + half_members - steps) % half_members

    def across(value):
        return lax.all_to_all(value, "fsdp", split_axis=0, concat_axis=0, tiled=True)

    def shifted(value, turn):
        pairs = [
            (i, i // half_members * half_members + (i + turn) % half_members)
            for i in range(members)
        ]
        return lax.ppermute(value, "fsdp", pairs)

    base = (group_index * per_group).astype(jnp.int32).reshape(1)
    table, count = route(base, assignment, members, most, per_group)
    slots = table.reshape(members, most)

    scaled, top = merge(expert_momentum, expert_grad)
    wide_merged, packed, squares = wide_gram(wide_momentum[0], wide_grad[0])
    notes = jnp.concatenate([top[:, 0, 0], squares[0, :1]])
    notes = jnp.pad(notes, (0, -notes.shape[0] % 128))
    notes = jnp.broadcast_to(notes[None, None, :], (members, 1, notes.shape[0]))
    notes = across(notes)[:, 0]
    coded = lax.optimization_barrier(scaled.astype(jnp.float16))
    arrived = []
    for start, chunk in zip(starts, sizes):
        picked = coded[slots[:, start:start + chunk].reshape(-1)]
        arrived.append(across(picked.reshape(members, chunk, rows, width)))

    packed_rows = packed.shape[0] // half_members
    packed = packed.reshape(half_members, packed_rows, BLOCK)
    parts = lax.all_to_all(
        packed, "fsdp", split_axis=0, concat_axis=0, tiled=True,
        axis_index_groups=[
            list(range(half_members)), list(range(half_members, members))
        ],
    )
    part = jnp.sum(parts.astype(F32), axis=0).astype(BF16)
    other = lax.ppermute(part, "fsdp", mirror)
    part = (part.astype(F32) + other.astype(F32)).astype(BF16)
    packed = [part] + [shifted(part, turn) for turn in range(1, half_members)]
    wide_norm = jnp.sum(notes[:, per_group]) + EPS
    coef = jnp.stack(
        [lax.rsqrt(wide_norm), 1.0 / wide_norm, jnp.float32(math.sqrt(wide_width * members))]
    )
    wide_out = wide_solve(coef, origin, packed, wide_merged)

    tops = notes[:, :per_group]
    keep = F16_TOP / jnp.minimum(2.0, jnp.max(tops, axis=0) * 2e7)
    tokens = expert_tokens.astype(F32)
    own_tokens = lax.dynamic_slice_in_dim(tokens, group_index * per_group, per_group)
    factor = jnp.sqrt(own_tokens / jnp.mean(tokens)) * math.sqrt(width)
    own_slots = lax.dynamic_index_in_dim(slots, me, 0, keepdims=False)
    half_slots = slots[half * half_members + origin]
    own_count = lax.dynamic_index_in_dim(count, me, 0, keepdims=False)
    own_pick = own_slots[:, None] == jnp.arange(per_group, dtype=jnp.int32)[None, :]
    half_pick = half_slots[:, :, None] == jnp.arange(per_group, dtype=jnp.int32)
    slot_scale = jnp.sum(jnp.where(own_pick[:, None, :], tops[None], 0.0), axis=2) / F16_TOP
    slot_keep = jnp.sum(jnp.where(own_pick, keep[None], 0.0), axis=1)
    slot_factor = jnp.sum(jnp.where(own_pick, factor[None], 0.0), axis=1)
    slot_ratio = slot_factor / slot_keep
    slot_factor = jnp.where(jnp.arange(most) < own_count, slot_factor, 0.0)
    home_factor = jnp.sum(jnp.where(half_pick, (factor / keep)[None, None], 0.0), axis=2)
    slot_scale = slot_scale.reshape(-1)
    row_starts = ((half * half_members + onward) * rows).astype(jnp.int32)

    work = None
    expert_out = None
    for index, piece in enumerate(arrived):
        start, chunk = starts[index], sizes[index]
        work, back = solve(
            row_starts, slot_scale, slot_keep, slot_factor, slot_ratio, piece.astype(F32), work,
            start, most, half_members,
        )
        received = []
        for turn in range(1, half_members):
            piece = shifted(back[turn].astype(jnp.float16), turn)
            received.append(piece.astype(F32) * home_factor[turn, start:start + chunk, None, None])
        ids = half_slots[:, start:start + chunk].reshape(-1)
        expert_out = home(ids, back, received, expert_out, per_group)
    return (expert_out, wide_out[None], work[None])


def solution(mesh):
    placed = (
        P("grp", "fsdp", None),
        P("grp", "fsdp", None),
        P("grp", None, "fsdp"),
        P("grp", None, "fsdp"),
        P(),
        P(),
    )
    return jax.shard_map(
        on_device,
        mesh=mesh,
        in_specs=placed,
        out_specs=(
            P("grp", "fsdp", None),
            P("grp", None, "fsdp"),
            P(("grp", "fsdp"), None, None, None),
        ),
        check_vma=False,
    )
```

```python
import functools
import math

import jax
import jax.numpy as jnp
from jax import lax
from jax.experimental import pallas as pl
from jax.experimental.pallas import tpu as pltpu
from jax.sharding import PartitionSpec as P


COEF_A = 3.4445
COEF_B = -4.775
COEF_C = 2.0315
BETA = 0.95
EPS = 1e-06

F16_TOP = 32768.0
SMALLEST = 1e-30
BLOCK = 256
PIECE = 128
SWEEP = 1024

F32 = jnp.float32
BF16 = jnp.bfloat16

SMEM_SPEC = pl.BlockSpec(memory_space=pltpu.SMEM)
ANY_SPEC = pl.BlockSpec(memory_space=pl.ANY)


def dot(left, right):
    return jnp.dot(left, right, preferred_element_type=F32)


def dot_nt(left, right):
    return lax.dot_general(left, right, (((1,), (1,)), ((), ())), preferred_element_type=F32)


def cost(flops, bytes_accessed):
    return pl.CostEstimate(flops=int(flops), bytes_accessed=int(bytes_accessed), transcendentals=0)


def route_kernel(members, most, per_group, base_ref, assign_ref, table_ref, count_ref):
    half_members = members // 2
    base = base_ref[0]
    for i in range(members * most):
        table_ref[i] = per_group - 1
    for j in range(members):
        count_ref[j] = 0

    def own(e, carry):
        worker = assign_ref[base + e]
        rank = count_ref[worker]
        table_ref[worker * most + rank] = e
        count_ref[worker] = rank + 1
        return carry

    lax.fori_loop(0, per_group, own, 0)
    for half in range(2):
        first = half * half_members
        last = first + half_members - 1

        def other(e, carry):
            holder, slot = carry
            worker = assign_ref[base + e]
            mine = jnp.logical_and(worker >= first, worker <= last)
            for _ in range(half_members - 1):
                full = slot >= most
                following = jnp.minimum(holder + 1, last)
                slot = jnp.where(full, count_ref[following], slot)
                holder = jnp.where(full, following, holder)

            @pl.when(jnp.logical_not(mine))
            def _():
                table_ref[holder * most + slot] = e

            return holder, jnp.where(mine, slot, slot + 1)

        lax.fori_loop(0, per_group, other, (jnp.int32(first), count_ref[first]))


def route(base, assignment, members, most, per_group):
    return pl.pallas_call(
        functools.partial(route_kernel, members, most, per_group),
        out_shape=(
            jax.ShapeDtypeStruct((members * most,), jnp.int32),
            jax.ShapeDtypeStruct((members,), jnp.int32),
        ),
        in_specs=[SMEM_SPEC, SMEM_SPEC],
        out_specs=(SMEM_SPEC, SMEM_SPEC),
        name="route",
    )(base, assignment)


def merge_kernel(momentum_ref, grad_ref, scaled_ref, top_ref):
    for i in range(momentum_ref.shape[0]):
        merged = BETA * momentum_ref[i] + grad_ref[i]
        top = jnp.maximum(jnp.max(jnp.abs(merged), keepdims=True), SMALLEST)
        scaled_ref[i] = merged * (F16_TOP / top)
        top_ref[i] = jnp.broadcast_to(top, top_ref.shape[1:])


def merge(momentum, grad):
    per_group, rows, width = momentum.shape
    step = 4
    spec = pl.BlockSpec((step, rows, width), lambda i: (i, 0, 0))
    return pl.pallas_call(
        merge_kernel,
        grid=(per_group // step,),
        out_shape=(
            jax.ShapeDtypeStruct(momentum.shape, F32),
            jax.ShapeDtypeStruct((per_group, 8, 128), F32),
        ),
        in_specs=[spec, spec],
        out_specs=(spec, pl.BlockSpec((step, 8, 128), lambda i: (i, 0, 0))),
        name="merge",
        cost_estimate=cost(5 * momentum.size, momentum.size * 12),
    )(momentum, grad)


def pick_kernel(table_ref, *refs):
    scaled_ref = refs[-1]
    for slot in range(scaled_ref.shape[1]):
        merged = BETA * refs[2 * slot][0] + refs[2 * slot + 1][0]
        top = jnp.maximum(jnp.max(jnp.abs(merged), keepdims=True), SMALLEST)
        scaled_ref[0, slot] = merged * (F16_TOP / top)


def pick_first(table, momentum, grad, members, most, chunk):
    rows, width = momentum.shape[1:]

    def source(slot):
        return pl.BlockSpec((1, rows, width), lambda i, table: (table[i * most + slot], 0, 0))

    return pl.pallas_call(
        pick_kernel,
        grid_spec=pltpu.PrefetchScalarGridSpec(
            num_scalar_prefetch=1,
            grid=(members,),
            in_specs=[source(slot) for slot in range(chunk) for _ in range(2)],
            out_specs=pl.BlockSpec((1, chunk, rows, width), lambda i, table: (i, 0, 0, 0)),
        ),
        out_shape=jax.ShapeDtypeStruct((members, chunk, rows, width), F32),
        name="pick_first",
        cost_estimate=cost(2e9, members * chunk * rows * width * 12),
    )(table, *([momentum, grad] * chunk))


def solve_kernel(
    members, half_members, first_slot,
    row_ref, scale_ref, keep_ref, factor_ref, ratio_ref, data_ref, *rest,
):
    work_ref, back_ref, whole, low = rest[-4:]
    rows = data_ref.shape[2]
    size, width = whole.shape
    slot = first_slot + pl.program_id(0)
    tile = min(512, width)

    for member in range(members):
        part = data_ref[member, 0] * scale_ref[slot * members + member]
        whole[pl.ds(member * rows, rows), :] = part
        low[pl.ds(member * rows, rows), :] = part.astype(BF16)

    gram = jnp.zeros((size, size), F32)
    for k in range(width // tile):
        block = low[:, k * tile:(k + 1) * tile]
        gram = gram + dot_nt(block, block)
    row_ids = lax.broadcasted_iota(jnp.int32, (size, size), 0)
    col_ids = lax.broadcasted_iota(jnp.int32, (size, size), 1)
    norm_sq = jnp.sum(jnp.where(row_ids == col_ids, gram, 0.0), keepdims=True) + EPS
    inverse = lax.rsqrt(norm_sq)
    g0 = gram / norm_sq
    g0_low = g0.astype(BF16)
    square = dot(g0_low, g0_low)
    cube = dot(g0_low, square.astype(BF16))
    u = COEF_B * g0 + COEF_C * square
    t = COEF_B * square + COEF_C * cube
    u_low = u.astype(BF16)
    g1 = (COEF_A * COEF_A) * g0 + (2 * COEF_A) * t + dot(u_low, t.astype(BF16))
    g1_low = g1.astype(BF16)
    v = COEF_B * g1 + COEF_C * dot(g1_low, g1_low)
    mix = (COEF_A * (u + v) + dot(v.astype(BF16), u_low)).astype(BF16)
    factor = factor_ref[slot]
    keep = keep_ref[slot]
    for k in range(width // tile):
        cols = slice(k * tile, (k + 1) * tile)
        moved = dot(mix, low[:, cols])
        result = ((COEF_A * COEF_A) * whole[:, cols] + moved) * inverse
        work_ref[0, :, cols] = result * factor
        whole[:, cols] = result * keep
    for turn in range(half_members):
        start = pl.multiple_of(row_ref[turn], rows)
        block = whole[pl.ds(start, rows), :]
        back_ref[turn, 0] = block * ratio_ref[slot] if turn == 0 else block


def solve(row_starts, scale, keep, factor, ratio, data, work, first_slot, most, half_members):
    members, chunk, rows, width = data.shape
    size = members * rows
    inputs = [row_starts, scale, keep, factor, ratio, data]
    specs = [SMEM_SPEC] * 5 + [pl.BlockSpec((members, 1, rows, width), lambda i: (0, i, 0, 0))]
    aliases = {}
    if work is not None:
        inputs.append(work)
        specs.append(ANY_SPEC)
        aliases = {6: 0}
    flops = chunk * (4 * size * size * width + 10 * size ** 3)
    return pl.pallas_call(
        functools.partial(solve_kernel, members, half_members, first_slot),
        grid=(chunk,),
        out_shape=(
            jax.ShapeDtypeStruct((most, size, width), F32),
            jax.ShapeDtypeStruct((half_members, chunk, rows, width), F32),
        ),
        in_specs=specs,
        out_specs=(
            pl.BlockSpec((1, size, width), lambda i: (first_slot + i, 0, 0)),
            pl.BlockSpec((half_members, 1, rows, width), lambda i: (0, i, 0, 0)),
        ),
        scratch_shapes=[
            pltpu.VMEM((size, width), F32),
            pltpu.VMEM((size, width), BF16),
        ],
        input_output_aliases=aliases,
        cost_estimate=cost(flops, data.size * 12),
    )(*inputs)


def home_kernel(half_members, ids_ref, local_ref, *rest):
    received = rest[:half_members - 1]
    out_ref, held, in_sem, out_sem = rest[-4:]
    chunk = local_ref.shape[1]
    loads, stores = [], []
    for turn in range(half_members):
        for slot in range(chunk):
            i = turn * chunk + slot
            source = received[turn - 1].at[slot] if turn else local_ref.at[0, slot]
            loads.append(pltpu.make_async_copy(source, held.at[i], in_sem.at[i]))
            loads[-1].start()
    for i, load in enumerate(loads):
        load.wait()
        stores.append(pltpu.make_async_copy(held.at[i], out_ref.at[ids_ref[i]], out_sem.at[i]))
        stores[-1].start()
    for store in stores:
        store.wait()


def home(ids, local, received, out, per_group):
    half_members, chunk, rows, width = local.shape
    number = half_members * chunk
    inputs = [ids, local] + received
    aliases = {}
    if out is not None:
        aliases = {len(inputs): 0}
        inputs.append(out)
    return pl.pallas_call(
        functools.partial(home_kernel, half_members),
        in_specs=[SMEM_SPEC] + [ANY_SPEC] * (len(inputs) - 1),
        out_specs=ANY_SPEC,
        out_shape=jax.ShapeDtypeStruct((per_group, rows, width), F32),
        scratch_shapes=[
            pltpu.VMEM((number, rows, width), F32),
            pltpu.SemaphoreType.DMA((number,)),
            pltpu.SemaphoreType.DMA((number,)),
        ],
        input_output_aliases=aliases,
        name="home",
        cost_estimate=cost(2e9, number * rows * width * 8),
    )(*inputs)


def wide_gram_kernel(momentum_ref, grad_ref, merged_ref, packed_ref, sum_ref, low):
    i = pl.program_id(0)
    step = 2 * BLOCK
    merged = BETA * momentum_ref[...] + grad_ref[...]
    merged_ref[...] = merged
    rounded = merged.astype(BF16)
    low[pl.ds(pl.multiple_of(i * step, step), step), :] = rounded

    @pl.when(i == 0)
    def _():
        sum_ref[...] = jnp.zeros_like(sum_ref)

    squares = jnp.square(rounded.astype(F32))
    sum_ref[...] += jnp.sum(squares, axis=(0, 1), keepdims=True)

    def columns(turn, carry):
        j = i - turn
        other = low[pl.ds(pl.multiple_of(j * step, step), step), :]
        product = dot_nt(rounded, other).astype(BF16)
        for a in range(2):
            row = 2 * i + a
            for b in range(2):
                place = pl.multiple_of((row * (row + 1) // 2 + 2 * j + b) * BLOCK, BLOCK)

                @pl.when(jnp.logical_or(turn > 0, b <= a))
                def _():
                    packed_ref[pl.ds(place, BLOCK), :] = product[
                        a * BLOCK:(a + 1) * BLOCK, b * BLOCK:(b + 1) * BLOCK
                    ]
        return carry

    lax.fori_loop(0, i + 1, columns, 0)


def wide_gram(momentum, grad):
    height, width = momentum.shape
    number = height // BLOCK
    packed = number * (number + 1) // 2 * BLOCK
    row_spec = pl.BlockSpec((2 * BLOCK, width), lambda i: (i, 0))
    return pl.pallas_call(
        wide_gram_kernel,
        grid=(number // 2,),
        out_shape=(
            jax.ShapeDtypeStruct((height, width), F32),
            jax.ShapeDtypeStruct((packed, BLOCK), BF16),
            jax.ShapeDtypeStruct((8, 128), F32),
        ),
        in_specs=[row_spec, row_spec],
        out_specs=(
            row_spec,
            pl.BlockSpec((packed, BLOCK), lambda i: (0, 0)),
            pl.BlockSpec((8, 128), lambda i: (0, 0)),
        ),
        scratch_shapes=[pltpu.VMEM((height, width), BF16)],
        name="wide_gram",
        cost_estimate=cost(packed * BLOCK * width * 2, height * width * 12 + packed * BLOCK * 2),
    )(momentum, grad)


def wide_solve_kernel(
    coef_ref, turn_ref, table_ref, merged_ref, *rest
):
    out_ref, packed_ref, gram, first, second, low, sem = rest[-7:]
    height, _ = out_ref.shape
    number = height // BLOCK
    pieces = packed_ref.shape[1] // PIECE
    loads = [
        pltpu.make_async_copy(piece, packed_ref.at[i], sem.at[i]) for i, piece in enumerate(rest[:-7])
    ]
    for load in loads:
        load.start()
    inverse, inverse_sq, outer = coef_ref[0], coef_ref[1], coef_ref[2]

    def prepare(i, carry):
        rows = pl.ds(pl.multiple_of(i * BLOCK, BLOCK), BLOCK)
        value = merged_ref[rows, :] * inverse
        first[rows, :] = value
        second[rows, :] = jnp.zeros_like(value)
        low[0, rows, :] = value.astype(BF16)
        return carry

    lax.fori_loop(0, number, prepare, 0)

    for load in loads:
        load.wait()

    def assemble(i, carry):
        rows = pl.ds(pl.multiple_of(i * BLOCK, BLOCK), BLOCK)

        def column(j, inner):
            cols = pl.ds(pl.multiple_of(j * BLOCK, BLOCK), BLOCK)
            found = []
            for p in range(BLOCK // PIECE):
                piece = (i * (i + 1) // 2 + j) * (BLOCK // PIECE) + p
                place = pl.multiple_of((piece % pieces) * PIECE, PIECE)
                found.append(packed_ref[turn_ref[piece // pieces], pl.ds(place, PIECE), :])
            block = jnp.concatenate(found, axis=0)
            gram[cols, rows] = block.T
            gram[rows, cols] = block
            return inner

        return lax.fori_loop(0, i + 1, column, carry)

    lax.fori_loop(0, number, assemble, 0)

    def sweep(step, carry):
        from_first, from_second, from_product = table_ref[step], table_ref[12 + step], table_ref[24 + step]
        now = step % 2

        def body(i, inner):
            rows = pl.ds(pl.multiple_of(i * SWEEP, SWEEP), SWEEP)
            product = dot(gram[rows, :], low[now]) * (inverse_sq * from_product)
            value = product + from_first * first[rows, :] + from_second * second[rows, :]

            @pl.when(step == 1)
            def _():
                first[rows, :] = value

            @pl.when(jnp.logical_or(step == 4, jnp.logical_or(step == 6, step == 9)))
            def _():
                second[rows, :] = value

            @pl.when(step == 11)
            def _():
                out_ref[rows, :] = value * outer

            low[1 - now, rows, :] = value.astype(BF16)
            return inner

        return lax.fori_loop(0, height // SWEEP, body, carry)

    lax.fori_loop(0, 12, sweep, 0)


A, B, C = COEF_A, COEF_B, COEF_C
SWEEP_FIRST = (B, A, B, A, 0, 0, B, 0, 0, 0, 0, A)
SWEEP_SECOND = (0, 0, 0, 0, 0, B, C * A, B, A, 0, B, A)
SWEEP_PRODUCT = (C, 1, C, 1, 1, C, C, C, 1, 1, C, 1)


def wide_solve(coef, turns, packed, merged):
    height, width = merged.shape
    number = len(packed)
    table = jnp.asarray(SWEEP_FIRST + SWEEP_SECOND + SWEEP_PRODUCT, F32)
    return pl.pallas_call(
        wide_solve_kernel,
        out_shape=jax.ShapeDtypeStruct((height, width), F32),
        in_specs=[SMEM_SPEC] * 3 + [pl.BlockSpec(memory_space=pltpu.VMEM)] + [ANY_SPEC] * number,
        out_specs=pl.BlockSpec(memory_space=pltpu.VMEM),
        scratch_shapes=[
            pltpu.VMEM((number,) + packed[0].shape, BF16),
            pltpu.VMEM((height, height), BF16),
            pltpu.VMEM((height, width), F32),
            pltpu.VMEM((height, width), F32),
            pltpu.VMEM((2, height, width), BF16),
            pltpu.SemaphoreType.DMA((number,)),
        ],
        name="wide_solve",
        cost_estimate=cost(24 * height * height * width, height * width * 8),
    )(coef, turns, table, merged, *packed)


def on_device(expert_momentum, expert_grad, wide_momentum, wide_grad, assignment, expert_tokens):
    members = lax.axis_size("fsdp")
    half_members = members // 2
    per_group, rows, width = expert_momentum.shape
    _, wide_width = wide_momentum.shape[1:]
    most = 2 * -(-per_group // members)
    sizes = [2, 1] * (most // 3) + [1] * (most % 3)
    starts = [sum(sizes[:i]) for i in range(len(sizes))]
    group_index = lax.axis_index("grp")
    me = lax.axis_index("fsdp")
    half = me // half_members
    place = me % half_members
    mirror = [(i, (i + half_members) % members) for i in range(members)]
    steps = jnp.arange(half_members, dtype=jnp.int32)
    onward = (place + steps) % half_members
    origin = (place + half_members - steps) % half_members

    def across(value):
        return lax.all_to_all(value, "fsdp", split_axis=0, concat_axis=0, tiled=True)

    def shifted(value, turn):
        pairs = [
            (i, i // half_members * half_members + (i + turn) % half_members)
            for i in range(members)
        ]
        return lax.ppermute(value, "fsdp", pairs)

    base = (group_index * per_group).astype(jnp.int32).reshape(1)
    table, count = route(base, assignment, members, most, per_group)
    slots = table.reshape(members, most)

    scaled, top = merge(expert_momentum, expert_grad)
    wide_merged, packed, squares = wide_gram(wide_momentum[0], wide_grad[0])
    notes = jnp.concatenate([top[:, 0, 0], squares[0, :1]])
    notes = jnp.pad(notes, (0, -notes.shape[0] % 128))
    notes = jnp.broadcast_to(notes[None, None, :], (members, 1, notes.shape[0]))
    notes = across(notes)[:, 0]
    coded = lax.optimization_barrier(scaled.astype(jnp.float16))
    arrived = []
    for index, (start, chunk) in enumerate(zip(starts, sizes)):
        if index == 0:
            picked = pick_first(table, expert_momentum, expert_grad, members, most, chunk)
            picked = picked.astype(jnp.float16)
        else:
            picked = coded[slots[:, start:start + chunk].reshape(-1)]
        arrived.append(across(picked.reshape(members, chunk, rows, width)))

    packed_rows = packed.shape[0] // half_members
    packed = packed.reshape(half_members, packed_rows, BLOCK)
    total = lax.dynamic_index_in_dim(packed, place, 0, keepdims=False).astype(F32)
    for turn in range(1, half_members):
        part = lax.dynamic_index_in_dim(packed, onward[turn], 0, keepdims=False)
        total = total + shifted(part, turn).astype(F32)
    part = total.astype(BF16)
    other = lax.ppermute(part, "fsdp", mirror)
    part = (part.astype(F32) + other.astype(F32)).astype(BF16)
    packed = [part] + [shifted(part, turn) for turn in range(1, half_members)]
    wide_norm = jnp.sum(notes[:, per_group]) + EPS
    coef = jnp.stack(
        [lax.rsqrt(wide_norm), 1.0 / wide_norm, jnp.float32(math.sqrt(wide_width * members))]
    )
    wide_out = wide_solve(coef, origin, packed, wide_merged)

    tops = notes[:, :per_group]
    keep = F16_TOP / jnp.minimum(2.0, jnp.max(tops, axis=0) * 2e7)
    tokens = expert_tokens.astype(F32)
    own_tokens = lax.dynamic_slice_in_dim(tokens, group_index * per_group, per_group)
    factor = jnp.sqrt(own_tokens / jnp.mean(tokens)) * math.sqrt(width)
    own_slots = lax.dynamic_index_in_dim(slots, me, 0, keepdims=False)
    half_slots = slots[half * half_members + origin]
    own_count = lax.dynamic_index_in_dim(count, me, 0, keepdims=False)
    own_pick = own_slots[:, None] == jnp.arange(per_group, dtype=jnp.int32)[None, :]
    half_pick = half_slots[:, :, None] == jnp.arange(per_group, dtype=jnp.int32)
    slot_scale = jnp.sum(jnp.where(own_pick[:, None, :], tops[None], 0.0), axis=2) / F16_TOP
    slot_keep = jnp.sum(jnp.where(own_pick, keep[None], 0.0), axis=1)
    slot_factor = jnp.sum(jnp.where(own_pick, factor[None], 0.0), axis=1)
    slot_ratio = slot_factor / slot_keep
    slot_factor = jnp.where(jnp.arange(most) < own_count, slot_factor, 0.0)
    home_factor = jnp.sum(jnp.where(half_pick, (factor / keep)[None, None], 0.0), axis=2)
    slot_scale = slot_scale.reshape(-1)
    row_starts = ((half * half_members + onward) * rows).astype(jnp.int32)

    work = None
    expert_out = None
    for index, piece in enumerate(arrived):
        start, chunk = starts[index], sizes[index]
        work, back = solve(
            row_starts, slot_scale, slot_keep, slot_factor, slot_ratio, piece.astype(F32), work,
            start, most, half_members,
        )
        received = []
        for turn in range(1, half_members):
            piece = shifted(back[turn].astype(jnp.float16), turn)
            received.append(piece.astype(F32) * home_factor[turn, start:start + chunk, None, None])
        ids = half_slots[:, start:start + chunk].reshape(-1)
        expert_out = home(ids, back, received, expert_out, per_group)
    return (expert_out, wide_out[None], work[None])


def solution(mesh):
    placed = (
        P("grp", "fsdp", None),
        P("grp", "fsdp", None),
        P("grp", None, "fsdp"),
        P("grp", None, "fsdp"),
        P(),
        P(),
    )
    return jax.shard_map(
        on_device,
        mesh=mesh,
        in_specs=placed,
        out_specs=(
            P("grp", "fsdp", None),
            P("grp", None, "fsdp"),
            P(("grp", "fsdp"), None, None, None),
        ),
        check_vma=False,
    )
```
